256 devices in a mesh: dp: 8 (over y, z_hi), fsdp: 32 (over x, z_lo, core).
Axes of the slice: x: 4, y: 4, z: 8 (z_hi: 2, z_lo: 4; z = z_hi * 4 + z_lo), core: 2. Of those that a mesh axis runs over, the one named last changes fastest.
Arguments:
- tokens: bfloat16 [98304, 1024], P(('dp', 'fsdp')), may hold values from -6.5 to 6.5
- cotangent: bfloat16 [98304, 1024], P(('dp', 'fsdp')), may hold values from -6 to 6
- patch_count: int32 [256], P(('dp', 'fsdp')), may hold values from 96 to 384, as said below
- image_starts: int32 [256, 8], P(('dp', 'fsdp')), may hold values from 0 to 384, as said below
- qkv_weight: bfloat16 [1024, 3072], P('fsdp'), may hold values from -8 to 8
- proj_weight: bfloat16 [1024, 1024], P('fsdp'), may hold values from -0.1875 to 0.1875
- norm_gain: bfloat16 [1024], P('fsdp'), may hold values from 0.25 to 1.75
- norm_shift: bfloat16 [1024], P('fsdp'), may hold values from -3 to 3
Outputs:
- grad_tokens: bfloat16 [98304, 1024], P(('dp', 'fsdp'))
- qkv_grad: float32 [1024, 3072], P('fsdp')
- proj_grad: float32 [1024, 1024], P('fsdp')
- gain_grad: float32 [1024], P('fsdp')
- shift_grad: float32 [1024], P('fsdp')
The draws below stay inside these ranges and needn't reach their ends.
Inputs may be any that keep to these rules, and one draw needn't show every extreme that they name: `patch_count`: at least one device has all 384 slots live; live slots of a device come first. `image_starts`: per device, non-decreasing and first 0; an image runs from its start to the next start or to the device's patch count; a start equal to the patch count marks an absent image; no image has more than 192 patches.
All inputs are finite; a program needn't handle non-finite values.
Results may differ from the reference program's by a relative error of at most 0.025.
The reference program's roundings to bfloat16 on the way count: a program that leaves them out, or rounds other values in their place, can miss the bound.
Values may be sent and summed in bfloat16 or wider, within the bound.
A program may use at most 128 MiB of HBM per device.

```python
import math
import jax
import jax.numpy as jnp
from jax import lax

D = 1024
HEAD_DIM = 64
HEADS = 16
TOK_DEV = 384
IMG_DEV = 8
TOKENS = 98304
N_DP = 8
N_FSDP = 32


def layout_draw(key):
    devices_all = N_DP * N_FSDP
    lengths = jax.random.randint(jax.random.fold_in(key, 11), (devices_all, IMG_DEV), TOK_DEV // 16 + 1, TOK_DEV // 2 + 1)
    limits = jax.random.randint(jax.random.fold_in(key, 12), (devices_all,), TOK_DEV // 4, TOK_DEV + 1)
    chosen = jax.random.randint(jax.random.fold_in(key, 13), (), 0, devices_all)
    picked = jnp.arange(devices_all, dtype=jnp.int32) == chosen
    limits = jnp.where(picked, TOK_DEV, limits)
    lengths = jnp.where(picked[:, None], TOK_DEV // 2, lengths)
    ends = jnp.cumsum(lengths, axis=1)
    starts = ends - lengths
    counts = jnp.minimum(ends[:, -1], limits).astype(jnp.int32)
    starts = jnp.minimum(starts, counts[:, None]).astype(jnp.int32)
    return (counts, starts)


def draw_patch_count(key, part):
    return layout_draw(key)[0]


def draw_image_starts(key, part):
    return layout_draw(key)[1]


def draw_tokens(key, part):
    base = jnp.clip(jax.random.normal(jax.random.fold_in(key, 21), (TOKENS, D), jnp.float32), -6.0, 6.0)
    return base.astype(jnp.bfloat16)


def draw_qkv_weight(key, part):
    base = jnp.clip(jax.random.normal(jax.random.fold_in(key, 31), (D, 3 * D), jnp.float32), -6.0, 6.0) * D ** (-0.5)
    return base.astype(jnp.bfloat16)


def block_scale(key, extent, cuts, least, top_value):
    factor_of, own = 1.0, jax.random.fold_in(key, 6)
    for axis_at, blocks in cuts:
        heights = jnp.exp(jax.random.uniform(jax.random.fold_in(own, axis_at), (blocks,), jnp.float32, least / len(cuts), top_value / len(cuts)))
        factor_of = factor_of * jnp.repeat(heights, extent[axis_at] // blocks).reshape([-1 if axis == axis_at else 1 for axis in range(len(extent))])
    return factor_of


def centred(own_key, extent, scale, limit, cuts=(), held_as=jnp.bfloat16):
    values = scale * jax.random.normal(own_key, extent, jnp.float32)
    if cuts:
        values = values * block_scale(own_key, extent, cuts, -0.22, 0.18)
    return jnp.clip(values, -limit, limit).astype(held_as)


def setup_inputs(seed: int = 0) -> dict:
    streams_of = jax.random.split(jax.random.key(seed), 9)
    return {
        "tokens": draw_tokens(jax.random.fold_in(streams_of[8], 71), 0),
        "cotangent": centred(streams_of[1], (TOKENS, D), 1.0, 6.0, ((0, 256),)),
        "patch_count": draw_patch_count(jax.random.fold_in(streams_of[8], 71), 0),
        "image_starts": draw_image_starts(jax.random.fold_in(streams_of[8], 71), 0),
        "qkv_weight": draw_qkv_weight(jax.random.fold_in(streams_of[8], 71), 0),
        "proj_weight": centred(streams_of[5], (D, D), D ** -0.5, 0.1875, ((0, 32),)),
        "norm_gain": jnp.clip(1.0 + 0.15 * jax.random.normal(streams_of[6], (D,), jnp.float32), 0.25, 1.75).astype(jnp.bfloat16),
        "norm_shift": centred(streams_of[7], (D,), 0.5, 3.0, ((0, 32),)),
    }


norm_eps = 1e-06
masked_score = -1e+30

def block_backward(block_tokens, block_cot, live_count, starts, qkv_weight, proj_weight, norm_gain, norm_shift):
    rows = block_tokens.shape[0]
    factor = HEAD_DIM ** (-0.5)
    position = jnp.arange(rows, dtype=jnp.int32)
    live = position < live_count
    segment = lax.optimization_barrier(jnp.sum((starts[None, :] <= position[:, None]).astype(jnp.int32), axis=1))
    allowed = live[:, None] & live[None, :] & (segment[:, None] == segment[None, :])
    source = block_tokens.astype(jnp.float32)
    center = lax.optimization_barrier(jnp.mean(source, axis=1, keepdims=True))
    centered = source - center
    variance = lax.optimization_barrier(jnp.mean(centered * centered, axis=1, keepdims=True))
    inverse = lax.rsqrt(variance + norm_eps)
    normed = centered * inverse
    gain = norm_gain.astype(jnp.float32)
    hidden = (normed * gain + norm_shift.astype(jnp.float32)).astype(jnp.bfloat16)
    qkv = jnp.dot(hidden, qkv_weight, preferred_element_type=jnp.float32).astype(jnp.bfloat16)
    split = qkv.reshape(rows, 3, HEADS, HEAD_DIM)
    queries = split[:, 0].astype(jnp.float32)
    keys = split[:, 1].astype(jnp.float32)
    values = split[:, 2].astype(jnp.float32)
    scores = jnp.einsum('qhe,khe->hqk', queries, keys) * factor
    scores = jnp.where(allowed[None], scores, masked_score)
    row_max = lax.optimization_barrier(jnp.max(scores, axis=2, keepdims=True))
    expon = jnp.exp(scores - row_max)
    probs = expon / lax.optimization_barrier(jnp.sum(expon, axis=2, keepdims=True))
    probs_low = probs.astype(jnp.bfloat16).astype(jnp.float32)
    attended = jnp.einsum('hqk,khe->qhe', probs_low, values).reshape(rows, D).astype(jnp.bfloat16)
    masked_cot = jnp.where(live[:, None], block_cot, jnp.zeros_like(block_cot))
    proj_term = jnp.dot(attended.T, masked_cot, preferred_element_type=jnp.float32)
    grad_attended = jnp.dot(masked_cot, proj_weight.T, preferred_element_type=jnp.float32).astype(jnp.bfloat16)
    grad_heads = grad_attended.reshape(rows, HEADS, HEAD_DIM).astype(jnp.float32)
    grad_probs = jnp.einsum('qhe,khe->hqk', grad_heads, values)
    grad_values = jnp.einsum('hqk,qhe->khe', probs_low, grad_heads).astype(jnp.bfloat16)
    grad_scores = probs * (grad_probs - lax.optimization_barrier(jnp.sum(probs * grad_probs, axis=2, keepdims=True))) * factor
    grad_scores = grad_scores.astype(jnp.bfloat16).astype(jnp.float32)
    grad_queries = jnp.einsum('hqk,khe->qhe', grad_scores, keys).astype(jnp.bfloat16)
    grad_keys = jnp.einsum('hqk,qhe->khe', grad_scores, queries).astype(jnp.bfloat16)
    grad_qkv = jnp.stack([grad_queries, grad_keys, grad_values], axis=1).reshape(rows, 3 * D)
    qkv_term = jnp.dot(hidden.T, grad_qkv, preferred_element_type=jnp.float32)
    grad_hidden = jnp.dot(grad_qkv, qkv_weight.T, preferred_element_type=jnp.float32)
    gain_term = lax.optimization_barrier(jnp.sum(grad_hidden * normed, axis=0))
    shift_term = lax.optimization_barrier(jnp.sum(grad_hidden, axis=0))
    grad_normed = grad_hidden * gain
    inner = grad_normed - lax.optimization_barrier(jnp.mean(grad_normed, axis=1, keepdims=True))
    inner = inner - normed * lax.optimization_barrier(jnp.mean(grad_normed * normed, axis=1, keepdims=True))
    grad_block = (block_cot.astype(jnp.float32) + inverse * inner).astype(jnp.bfloat16)
    return (grad_block, qkv_term, proj_term, gain_term, shift_term)

def reference(tokens, cotangent, patch_count, image_starts, qkv_weight, proj_weight, norm_gain, norm_shift):
    device_count = patch_count.shape[0]
    token_blocks = tokens.reshape(device_count, TOK_DEV, D)
    cot_blocks = cotangent.reshape(device_count, TOK_DEV, D)

    def visit(totals, inputs):
        block_tokens, block_cot, live_count, starts = inputs
        grad_block, qkv_term, proj_term, gain_term, shift_term = block_backward(block_tokens, block_cot, live_count, starts, qkv_weight, proj_weight, norm_gain, norm_shift)
        totals = (totals[0] + qkv_term, totals[1] + proj_term, totals[2] + gain_term, totals[3] + shift_term)
        return (totals, grad_block)
    start_totals = (jnp.zeros((D, 3 * D), jnp.float32), jnp.zeros((D, D), jnp.float32), jnp.zeros((D,), jnp.float32), jnp.zeros((D,), jnp.float32))
    totals, grad_blocks = lax.scan(visit, start_totals, (token_blocks, cot_blocks, patch_count, image_starts))
    factor = 1.0 / math.sqrt(TOKENS)
    return (grad_blocks.reshape(TOKENS, D), totals[0] * factor, totals[1] * factor, totals[2] * factor, totals[3] * factor)
```

```python
import functools
import math

import jax
import jax.numpy as jnp
from jax import lax
from jax.experimental import pallas as pl
from jax.experimental.pallas import tpu as pltpu
from jax.sharding import PartitionSpec as P

D = 1024
HEAD_DIM = 64
HEADS = 16
MESH = pl.DeviceIdType.MESH
F32 = jnp.float32
BF16 = jnp.bfloat16

norm_eps = 1e-06
masked_score = -1e30


class Place:
    def __init__(self):
        dp, fsdp = lax.axis_index("dp"), lax.axis_index("fsdp")
        self.dp, self.fsdp = dp, fsdp
        self.y, self.zhi = dp // 2, dp % 2
        self.c = fsdp % 2
        chip = fsdp // 2
        self.x, self.zlo = chip // 4, chip % 4
        self.z = self.zhi * 4 + self.zlo

    def at(self, dx=0, dy=0, dz=0, flip=0):
        x = (self.x + dx + 4) % 4
        y = (self.y + dy + 4) % 4
        z = (self.z + dz + 8) % 8
        c = self.c + flip * (1 - 2 * self.c)
        return {"dp": y * 2 + z // 4, "fsdp": (x * 4 + z % 4) * 2 + c}

    def along_x(self, d):
        return self.at(dx=(1 - self.c) * d, dz=self.c * d)

    def along_z(self, d):
        return self.at(dx=self.c * d, dz=(1 - self.c) * d)

    def chip(self, i, j):
        x = (self.x + (1 - self.c) * i + self.c * j + 8) % 4
        z = (self.zlo + self.c * i + (1 - self.c) * j + 8) % 4
        return x * 4 + z

    def sibling(self):
        return self.at(flip=1)

    def partner(self):
        return self.at(dz=4)


def enter(devices):
    barrier = pltpu.get_barrier_semaphore()
    for device in devices:
        pl.semaphore_signal(barrier, inc=1, device_id=device, device_id_type=MESH)
    pl.semaphore_wait(barrier, len(devices))


def send(src, dst, send_sem, recv_sem, device):
    return pltpu.make_async_remote_copy(
        src_ref=src,
        dst_ref=dst,
        send_sem=send_sem,
        recv_sem=recv_sem,
        device_id=device,
        device_id_type=MESH,
    )


GATHER_SEMS = 36


class Gather:
    def __init__(self, place, buffer, send_sems, recv_sems):
        self.place, self.buffer = place, buffer
        self.send_sems, self.recv_sems = send_sems, recv_sems
        self.sent = []

    def block(self, i, j, rows=None):
        ref = self.buffer.at[self.place.chip(i, j), self.place.c]
        return ref if rows is None else ref.at[pl.ds(rows * 16, 16)]

    def copy(self, src, index, device):
        return send(src, src, self.send_sems.at[index], self.recv_sems.at[index], device)

    def start(self, src, index, device):
        copy = self.copy(src, index, device)
        copy.start()
        self.sent.append(copy)

    def arrived(self, ref, index):
        self.copy(ref, index, self.place.sibling()).wait_recv()

    def to_second(self, i):
        at = self.place
        self.start(self.block(i, 0), 4 + 4 * (i % 4), at.along_z(1))
        self.start(self.block(i, 0), 5 + 4 * (i % 4), at.along_z(-1))
        self.to_sibling(i, 0)

    def to_sibling(self, i, j):
        self.start(self.block(i, j), 20 + 4 * (i % 4) + (j % 4), self.place.sibling())

    def stage0(self):
        at = self.place
        self.start(self.block(0, 0), 0, at.along_x(1))
        self.start(self.block(0, 0), 1, at.along_x(-1))
        self.to_second(0)

    def stage1(self):
        at = self.place
        self.arrived(self.block(-1, 0), 0)
        self.start(self.block(-1, 0, 0), 2, at.along_x(1))
        self.arrived(self.block(1, 0), 1)
        self.start(self.block(1, 0, 1), 3, at.along_x(-1))
        self.to_second(-1)
        self.to_second(1)

    def stage2(self):
        self.arrived(self.block(2, 0, 0), 2)
        self.arrived(self.block(2, 0, 1), 3)
        self.to_second(2)

    def stage3(self, i):
        at = self.place
        k = i % 4
        self.arrived(self.block(i, -1), 4 + 4 * k)
        self.start(self.block(i, -1, 0), 6 + 4 * k, at.along_z(1))
        self.to_sibling(i, -1)
        self.arrived(self.block(i, 1), 5 + 4 * k)
        self.start(self.block(i, 1, 1), 7 + 4 * k, at.along_z(-1))
        self.to_sibling(i, 1)

    def stage4(self, i):
        k = i % 4
        self.arrived(self.block(i, 2, 0), 6 + 4 * k)
        self.arrived(self.block(i, 2, 1), 7 + 4 * k)
        self.to_sibling(i, 2)

    def stage5(self):
        at = self.place
        for i in range(4):
            for j in range(4):
                ref = self.buffer.at[at.chip(j, i), 1 - at.c]
                self.arrived(ref, 20 + 4 * i + j)
        for copy in self.sent:
            copy.wait_send()

    def neighbours(self):
        at = self.place
        return [at.along_x(1), at.along_x(-1), at.along_z(1), at.along_z(-1), at.sibling()]


ORDER = (0, -1, 1, 2)


def gather_kernel(qkv_ref, proj_ref, small_ref, qkv_out, proj_out, small_out, *scratch):
    place = Place()
    sems = scratch[-3:]
    buffers = scratch[:-3]
    own = (qkv_ref, proj_ref, small_ref)
    outs = (qkv_out, proj_out, small_out)
    me = place.chip(0, 0)
    local = []
    for k, (src, buffer) in enumerate(zip(own, buffers)):
        copy = pltpu.make_async_copy(src, buffer.at[me, place.c], sems[2].at[k])
        copy.start()
        local.append(copy)
    pieces = [
        Gather(place, buffer, sems[0].at[k], sems[1].at[k]) for k, buffer in enumerate(buffers)
    ]
    enter(pieces[0].neighbours())
    for copy, piece in zip(local, pieces):
        copy.wait()
        piece.stage0()
    for piece in pieces:
        piece.stage1()
    for piece in pieces:
        piece.stage2()
    for i in ORDER:
        for piece in pieces:
            piece.stage3(i)
    for i in ORDER:
        for piece in pieces:
            piece.stage4(i)
    done = []
    for k, (piece, out) in enumerate(zip(pieces, outs)):
        piece.stage5()
        copy = pltpu.make_async_copy(piece.buffer, out, sems[2].at[k])
        copy.start()
        done.append(copy)
    for copy in done:
        copy.wait()


def gather(qkv_weight, proj_weight, small):
    widths = (3072, 1024, 128)
    anyspace = pl.BlockSpec(memory_space=pl.ANY)
    shapes = [(16, 2, 32, w) for w in widths]
    outs = pl.pallas_call(
        gather_kernel,
        out_shape=[jax.ShapeDtypeStruct(s, BF16) for s in shapes],
        in_specs=[anyspace] * 3,
        out_specs=[anyspace] * 3,
        scratch_shapes=[pltpu.VMEM(s, BF16) for s in shapes]
        + [
            pltpu.SemaphoreType.DMA((3, GATHER_SEMS)),
            pltpu.SemaphoreType.DMA((3, GATHER_SEMS)),
            pltpu.SemaphoreType.DMA((3,)),
        ],
        compiler_params=pltpu.CompilerParams(collective_id=0, has_side_effects=True),
        name="gather",
    )(qkv_weight, proj_weight, small)
    return [o.reshape(D, w) for o, w in zip(outs, widths)]


REDUCE_SEMS = 17


def reduce_shapes(width):
    half = width // 2
    return dict(
        R=(4, 4, 2, 2, 16, half),
        A=(4, 4, 4, 16, half),
        T=(2, 2, 4, 16, half),
        U=(2, 4, 4, 16, half),
        B=(4, 4, 16, half),
        Y=(3, 4, 16, half),
        C=(4, 16, half),
        V=(3, 16, half),
        E=(2, 16, half),
        Z=(16, half),
        O=(4, 16, half),
    )


class Reduce:
    def __init__(self, place, term, width, buffers, send_sems, recv_sems):
        self.place, self.term, self.half = place, term, width // 2
        for name, ref in buffers.items():
            setattr(self, name, ref)
        self.send_sems, self.recv_sems = send_sems, recv_sems
        self.sent = []

    def copy(self, src, dst, index, device):
        return send(src, dst, self.send_sems.at[index], self.recv_sems.at[index], device)

    def start(self, src, dst, index, device):
        copy = self.copy(src, dst, index, device)
        copy.start()
        self.sent.append(copy)

    def arrived(self, ref, index):
        self.copy(ref, ref, index, self.place.sibling()).wait_recv()

    def finish(self):
        for copy in self.sent:
            copy.wait_send()

    def stage0(self):
        at = self.place
        self.start(self.term.at[:, :, 1 - at.c], self.R, 0, at.sibling())

    def pair(self, d1):
        at = self.place
        for d3 in range(4):
            chip = at.chip(d3, d1)
            x, z = chip // 4, chip % 4
            both = self.term[x, z, at.c].astype(F32) + self.R[x, z].astype(F32)
            self.A[d1, d3] = both.astype(BF16).reshape(4, 16, self.half)

    def stage1(self):
        at = self.place
        self.arrived(self.R, 0)
        self.pair(2)
        self.start(self.A.at[2, pl.ds(0, 2)], self.T.at[0], 1, at.along_z(1))
        self.start(self.A.at[2, pl.ds(2, 2)], self.T.at[1], 2, at.along_z(-1))
        self.pair(1)
        self.pair(3)
        self.pair(0)

    def stage2(self):
        at = self.place
        self.arrived(self.T.at[0], 1)
        self.A[1, 0:2] = (self.A[1, 0:2].astype(F32) + self.T[0].astype(F32)).astype(BF16)
        self.start(self.A.at[1], self.U.at[0], 3, at.along_z(1))
        self.arrived(self.T.at[1], 2)
        self.A[3, 2:4] = (self.A[3, 2:4].astype(F32) + self.T[1].astype(F32)).astype(BF16)
        self.start(self.A.at[3], self.U.at[1], 4, at.along_z(-1))

    def stage3(self):
        at = self.place
        self.arrived(self.U.at[0], 3)
        self.arrived(self.U.at[1], 4)
        for d3 in range(4):
            total = self.A[0, d3].astype(F32) + self.U[0, d3].astype(F32)
            self.B[d3] = (total + self.U[1, d3].astype(F32)).astype(BF16)
        for d2 in (2, 1, 3):
            q = (at.y + d2) % 4
            self.start(self.B.at[:, q], self.Y.at[d2 - 1], 4 + d2, at.at(dy=d2))

    def stage4(self):
        at = self.place
        for d2 in (1, 3, 2):
            self.arrived(self.Y.at[d2 - 1], 4 + d2)
        for d3 in (2, 1, 3, 0):
            total = self.B[d3, at.y].astype(F32) + self.Y[0, d3].astype(F32)
            total = total + self.Y[1, d3].astype(F32) + self.Y[2, d3].astype(F32)
            self.C[d3] = total.astype(BF16)
        low, high = pl.ds(0, 128), pl.ds(128, self.half - 128)
        self.start(self.C.at[2, :, low], self.V.at[1, :, low], 8, at.along_x(2))
        self.start(self.C.at[2, :, high], self.V.at[1, :, high], 9, at.along_x(-2))
        self.start(self.C.at[1], self.V.at[0], 10, at.along_x(1))
        self.start(self.C.at[3], self.V.at[2], 11, at.along_x(-1))

    def stage5(self):
        at = self.place
        low, high = pl.ds(0, 128), pl.ds(128, self.half - 128)
        self.arrived(self.V.at[0], 10)
        self.arrived(self.V.at[2], 11)
        self.arrived(self.V.at[1, :, low], 8)
        self.arrived(self.V.at[1, :, high], 9)
        total = self.C[0].astype(F32) + self.V[0].astype(F32)
        total = total + self.V[1].astype(F32) + self.V[2].astype(F32)
        self.E[0] = total.astype(BF16)
        self.start(self.E.at[0], self.Z, 12, at.partner())

    def stage6(self):
        at = self.place
        self.arrived(self.Z, 12)
        total = (self.E[0].astype(F32) + self.Z[...].astype(F32)).astype(BF16)
        self.E[1] = total
        for d2 in (2, 1, 3):
            self.start(self.E.at[1], self.O.at[at.y], 12 + d2, at.at(dy=d2))

    def stage7(self, write):
        at = self.place
        for d2 in (1, 3, 2):
            self.arrived(self.O.at[(at.y - d2 + 4) % 4], 12 + d2)
        self.O[at.y] = self.E[1]
        for r in range(2):
            for k in range(2):
                write(r, k, self.O[2 * r + k].astype(F32))

    def neighbours(self):
        at = self.place
        return (
            [at.sibling(), at.partner()]
            + [at.along_z(1), at.along_z(-1)]
            + [at.along_x(d) for d in (1, -1, 2, -2)]
            + [at.at(dy=d) for d in (1, 2, 3)]
        )


REDUCE_PIECES = ((0, 0, 768), (0, 768, 768), (0, 1536, 768), (0, 2304, 768), (1, 0, 1024), (2, 0, 512))


def reduce_kernel(names, scale, *refs):
    ins, outs, scratch = refs[:3], refs[3:6], refs[6:]
    place = Place()
    per = 1 + len(names)
    count = len(REDUCE_PIECES)
    sems = scratch[per * count :]
    pieces, local = [], []
    for n, (which, start, width) in enumerate(REDUCE_PIECES):
        term = scratch[n * per]
        buffers = dict(zip(names, scratch[n * per + 1 : (n + 1) * per]))
        pieces.append(Reduce(place, term, width, buffers, sems[0].at[n], sems[1].at[n]))
        for k in range(2):
            half = width // 2
            copy = pltpu.make_async_copy(
                ins[which].at[:, :, :, :, :, pl.ds(start + k * half, half)],
                term.at[:, :, :, :, k],
                sems[2].at[n, k],
            )
            copy.start()
            local.append(copy)
    enter(pieces[0].neighbours())
    for n, piece in enumerate(pieces):
        local[2 * n].wait()
        local[2 * n + 1].wait()
        piece.stage0()

    def writer(n):
        which, start, width = REDUCE_PIECES[n]
        half = width // 2

        def write(r, k, value):
            outs[which][r * 16 : r * 16 + 16, start + k * half : start + (k + 1) * half] = (
                value * scale
            )

        return write

    for slot in range(count + 6):
        for n, piece in enumerate(pieces):
            stage = slot - n + 1
            if stage == 7:
                piece.stage7(writer(n))
            elif 1 <= stage < 7:
                getattr(piece, f"stage{stage}")()
    for piece in pieces:
        piece.finish()


def reduce(qkv_term, proj_term, small_term, scale):
    scratch = []
    for _, _, width in REDUCE_PIECES:
        shapes = reduce_shapes(width)
        scratch.append(pltpu.VMEM((4, 4, 2, 2, 2, 16, width // 2), BF16))
        scratch += [pltpu.VMEM(s, BF16) for s in shapes.values()]
    count = len(REDUCE_PIECES)
    anyspace = pl.BlockSpec(memory_space=pl.ANY)
    vmem = pl.BlockSpec(memory_space=pltpu.VMEM)
    widths = (3072, 1024, 512)
    terms = [
        t.reshape(4, 4, 2, 2, 16, w) for t, w in zip((qkv_term, proj_term, small_term), widths)
    ]
    return pl.pallas_call(
        functools.partial(reduce_kernel, tuple(shapes), scale),
        out_shape=[jax.ShapeDtypeStruct((32, w), F32) for w in widths],
        in_specs=[anyspace] * 3,
        out_specs=[vmem] * 3,
        scratch_shapes=scratch
        + [
            pltpu.SemaphoreType.DMA((count, REDUCE_SEMS)),
            pltpu.SemaphoreType.DMA((count, REDUCE_SEMS)),
            pltpu.SemaphoreType.DMA((count, 2)),
        ],
        compiler_params=pltpu.CompilerParams(
            collective_id=1, has_side_effects=True, vmem_limit_bytes=56 * 2**20
        ),
        name="reduce",
    )(*terms)


def block_backward(
    block_tokens, block_cot, live_count, starts, qkv_weight, proj_weight, norm_gain, norm_shift
):
    rows = block_tokens.shape[0]
    factor = HEAD_DIM ** (-0.5)
    position = jnp.arange(rows, dtype=jnp.int32)
    live = position < live_count
    segment = jnp.sum((starts[None, :] <= position[:, None]).astype(jnp.int32), axis=1)
    allowed = live[:, None] & live[None, :] & (segment[:, None] == segment[None, :])
    source = block_tokens.astype(jnp.float32)
    center = jnp.mean(source, axis=1, keepdims=True)
    centered = source - center
    variance = jnp.mean(centered * centered, axis=1, keepdims=True)
    inverse = lax.rsqrt(variance + norm_eps)
    normed = centered * inverse
    gain = norm_gain.astype(jnp.float32)
    hidden = (normed * gain + norm_shift.astype(jnp.float32)).astype(jnp.bfloat16)
    qkv = jnp.dot(hidden, qkv_weight, preferred_element_type=jnp.float32).astype(jnp.bfloat16)
    split = qkv.reshape(rows, 3, HEADS, HEAD_DIM)
    queries = split[:, 0]
    keys = split[:, 1]
    values = split[:, 2]
    scores = jnp.einsum("qhe,khe->hqk", queries, keys, preferred_element_type=jnp.float32) * factor
    scores = jnp.where(allowed[None], scores, masked_score)
    row_max = jnp.max(scores, axis=2, keepdims=True)
    expon = jnp.exp(scores - row_max)
    probs = expon / jnp.sum(expon, axis=2, keepdims=True)
    probs_low = probs.astype(jnp.bfloat16)
    attended = (
        jnp.einsum("hqk,khe->qhe", probs_low, values, preferred_element_type=jnp.float32)
        .reshape(rows, D)
        .astype(jnp.bfloat16)
    )
    masked_cot = jnp.where(live[:, None], block_cot, jnp.zeros_like(block_cot))
    proj_term = jnp.dot(attended.T, masked_cot, preferred_element_type=jnp.float32)
    grad_attended = jnp.dot(masked_cot, proj_weight.T, preferred_element_type=jnp.float32).astype(
        jnp.bfloat16
    )
    grad_heads = grad_attended.reshape(rows, HEADS, HEAD_DIM)
    grad_probs = jnp.einsum("qhe,khe->hqk", grad_heads, values, preferred_element_type=jnp.float32)
    grad_values = jnp.einsum(
        "hqk,qhe->khe", probs_low, grad_heads, preferred_element_type=jnp.float32
    ).astype(jnp.bfloat16)
    grad_scores = probs * (grad_probs - jnp.sum(probs * grad_probs, axis=2, keepdims=True)) * factor
    grad_scores = grad_scores.astype(jnp.bfloat16)
    grad_queries = jnp.einsum(
        "hqk,khe->qhe", grad_scores, keys, preferred_element_type=jnp.float32
    ).astype(jnp.bfloat16)
    grad_keys = jnp.einsum(
        "hqk,qhe->khe", grad_scores, queries, preferred_element_type=jnp.float32
    ).astype(jnp.bfloat16)
    grad_qkv = jnp.stack([grad_queries, grad_keys, grad_values], axis=1).reshape(rows, 3 * D)
    qkv_term = jnp.dot(hidden.T, grad_qkv, preferred_element_type=jnp.float32)
    grad_hidden = jnp.dot(grad_qkv, qkv_weight.T, preferred_element_type=jnp.float32)
    gain_term = jnp.sum(grad_hidden * normed, axis=0)
    shift_term = jnp.sum(grad_hidden, axis=0)
    grad_normed = grad_hidden * gain
    inner = grad_normed - jnp.mean(grad_normed, axis=1, keepdims=True)
    inner = inner - normed * jnp.mean(grad_normed * normed, axis=1, keepdims=True)
    grad_block = (block_cot.astype(jnp.float32) + inverse * inner).astype(jnp.bfloat16)
    return (grad_block, qkv_term, proj_term, gain_term, shift_term)


def per_device(
    tokens, cotangent, patch_count, image_starts, qkv_weight, proj_weight, norm_gain, norm_shift
):
    small = jnp.pad(jnp.stack([norm_gain, norm_shift], axis=1), ((0, 0), (0, 126)))
    whole_qkv, whole_proj, whole_small = gather(qkv_weight, proj_weight, small)
    grad_block, qkv_term, proj_term, gain_term, shift_term = block_backward(
        tokens,
        cotangent,
        patch_count[0],
        image_starts[0],
        whole_qkv,
        whole_proj,
        whole_small[:, 0],
        whole_small[:, 1],
    )
    replicas = lax.axis_size("dp")
    owners = lax.axis_size("fsdp")
    scale = 1.0 / math.sqrt(tokens.shape[0] * replicas * owners)
    small_term = jnp.pad(jnp.stack([gain_term, shift_term], axis=1), ((0, 0), (0, 510)))
    qkv_grad, proj_grad, small_grad = reduce(
        qkv_term.astype(BF16), proj_term.astype(BF16), small_term.astype(BF16), scale
    )
    return (grad_block, qkv_grad, proj_grad, small_grad[:, 0], small_grad[:, 1])


def solution(mesh):
    placed = (
        P(("dp", "fsdp"), None),
        P(("dp", "fsdp"), None),
        P(("dp", "fsdp")),
        P(("dp", "fsdp"), None),
        P("fsdp", None),
        P("fsdp", None),
        P("fsdp"),
        P("fsdp"),
    )
    return jax.shard_map(
        per_device,
        mesh=mesh,
        in_specs=placed,
        out_specs=(P(("dp", "fsdp"), None), P("fsdp", None), P("fsdp", None), P("fsdp"), P("fsdp")),
        check_vma=False,
    )
```

```python
import functools
import math

import jax
import jax.numpy as jnp
from jax import lax
from jax.experimental import pallas as pl
from jax.experimental.pallas import tpu as pltpu
from jax.sharding import PartitionSpec as P

MESH = pl.DeviceIdType.MESH
F32 = jnp.float32
BF16 = jnp.bfloat16
D = 1024
ROWS = 384


def nn(a, b):
    return lax.dot_general(a, b, (((1,), (0,)), ((), ())), preferred_element_type=F32)


def nt(a, b):
    return lax.dot_general(a, b, (((1,), (1,)), ((), ())), preferred_element_type=F32)


def tn(a, b):
    return lax.dot_general(a, b, (((0,), (0,)), ((), ())), preferred_element_type=F32)


class Place:
    def __init__(self):
        dp, fsdp = lax.axis_index("dp"), lax.axis_index("fsdp")
        self.y, self.zhi = dp // 2, dp % 2
        self.c = fsdp % 2
        chip = fsdp // 2
        self.x, self.zlo = chip // 4, chip % 4
        self.z = self.zhi * 4 + self.zlo

    def at(self, dx=0, dy=0, dz=0, flip=0):
        x = (self.x + dx + 4) % 4
        y = (self.y + dy + 4) % 4
        z = (self.z + dz + 8) % 8
        c = self.c + flip * (1 - 2 * self.c)
        return {"dp": y * 2 + z // 4, "fsdp": (x * 4 + z % 4) * 2 + c}

    def along_x(self, d):
        return self.at(dx=(1 - self.c) * d, dz=self.c * d)

    def along_z(self, d):
        return self.at(dx=self.c * d, dz=(1 - self.c) * d)

    def chip(self, i, j):
        x = (self.x + (1 - self.c) * i + self.c * j + 8) % 4
        z = (self.zlo + self.c * i + (1 - self.c) * j + 8) % 4
        return x, z

    def sibling(self):
        return self.at(flip=1)

    def partner(self):
        return self.at(dz=4)

    def all(self):
        return (
            [self.sibling(), self.partner()]
            + [self.along_z(1), self.along_z(-1)]
            + [self.along_x(d) for d in (1, -1, 2, -2)]
            + [self.at(dy=d) for d in (1, 2, 3)]
        )


def enter(devices):
    barrier = pltpu.get_barrier_semaphore()
    for device in devices:
        pl.semaphore_signal(barrier, inc=1, device_id=device, device_id_type=MESH)
    pl.semaphore_wait(barrier, len(devices))


class Copies:
    def __init__(self, place, send_sems, recv_sems):
        self.place, self.send_sems, self.recv_sems = place, send_sems, recv_sems

    def copy(self, src, dst, n, device):
        return pltpu.make_async_remote_copy(
            src_ref=src,
            dst_ref=dst,
            send_sem=self.send_sems.at[n],
            recv_sem=self.recv_sems.at[n],
            device_id=device,
            device_id_type=MESH,
        )

    def start(self, src, dst, n, device):
        self.copy(src, dst, n, device).start()

    def arrived(self, ref, n):
        self.copy(ref, ref, n, self.place.sibling()).wait_recv()

    def left(self, ref, n):
        self.copy(ref, ref, n, self.place.sibling()).wait_send()


GATHER_SEMS = 36
ORDER = (0, -1, 1, 2)


class Gather(Copies):
    def __init__(self, place, buffer, send_sems, recv_sems):
        super().__init__(place, send_sems, recv_sems)
        self.buffer = buffer

    def block(self, i, j, half=None):
        x, z = self.place.chip(i, j)
        ref = self.buffer.at[x, z, self.place.c]
        return ref if half is None else ref.at[pl.ds(half * 16, 16)]

    def forward(self, ref, n, device):
        self.start(ref, ref, n, device)

    def to_second(self, i):
        self.forward(self.block(i, 0), 4 + 4 * (i % 4), self.place.along_z(1))
        self.forward(self.block(i, 0), 5 + 4 * (i % 4), self.place.along_z(-1))
        self.to_sibling(i, 0)

    def to_sibling(self, i, j):
        self.forward(self.block(i, j), 20 + 4 * (i % 4) + (j % 4), self.place.sibling())

    def stage0(self):
        self.forward(self.block(0, 0), 0, self.place.along_x(1))
        self.forward(self.block(0, 0), 1, self.place.along_x(-1))
        self.to_second(0)

    def stage1(self):
        self.arrived(self.block(-1, 0), 0)
        self.forward(self.block(-1, 0, 0), 2, self.place.along_x(1))
        self.arrived(self.block(1, 0), 1)
        self.forward(self.block(1, 0, 1), 3, self.place.along_x(-1))
        self.to_second(-1)
        self.to_second(1)

    def stage2(self):
        self.arrived(self.block(2, 0, 0), 2)
        self.arrived(self.block(2, 0, 1), 3)
        self.to_second(2)

    def stage3(self):
        for i in ORDER:
            k = i % 4
            self.arrived(self.block(i, -1), 4 + 4 * k)
            self.forward(self.block(i, -1, 0), 6 + 4 * k, self.place.along_z(1))
            self.to_sibling(i, -1)
            self.arrived(self.block(i, 1), 5 + 4 * k)
            self.forward(self.block(i, 1, 1), 7 + 4 * k, self.place.along_z(-1))
            self.to_sibling(i, 1)

    def stage4(self):
        for i in ORDER:
            k = i % 4
            self.arrived(self.block(i, 2, 0), 6 + 4 * k)
            self.arrived(self.block(i, 2, 1), 7 + 4 * k)
            self.to_sibling(i, 2)

    def stage5(self):
        for i in range(4):
            for j in range(4):
                x, z = self.place.chip(j, i)
                self.arrived(self.buffer.at[x, z, 1 - self.place.c], 20 + 4 * i + j)

    def drain(self):
        whole, half = self.block(0, 0), self.block(0, 0, 0)
        for n in range(GATHER_SEMS):
            self.left(half if n in (2, 3) or (n < 20 and n % 4 > 1) else whole, n)


REDUCE_SEMS = 16


def reduce_shapes(width):
    half = width // 2
    return dict(
        R=(4, 4, 2, 2, 16, half),
        A=(4, 4, 4, 16, half),
        T=(2, 2, 4, 16, half),
        U=(2, 4, 4, 16, half),
        B=(4, 4, 16, half),
        Y=(3, 4, 16, half),
        C=(4, 16, half),
        V=(3, 16, half),
        E=(2, 16, half),
        Z=(16, half),
        O=(4, 16, half),
    )


REDUCE_NAMES = tuple(reduce_shapes(256))


class Reduce(Copies):
    def __init__(self, place, term, buffers, half, send_sems, recv_sems):
        super().__init__(place, send_sems, recv_sems)
        self.term, self.half = term, half
        for name, ref in zip(REDUCE_NAMES, buffers):
            setattr(self, name, ref)
        self.low, self.high = pl.ds(0, 128), pl.ds(128, half - 128)

    def stage0(self):
        self.start(self.term.at[:, :, 1 - self.place.c], self.R, 0, self.place.sibling())

    def pair(self, d1):
        for d3 in range(4):
            x, z = self.place.chip(d3, d1)
            both = self.term[x, z, self.place.c].astype(F32) + self.R[x, z].astype(F32)
            self.A[d1, d3] = both.astype(BF16).reshape(4, 16, self.half)

    def stage1(self):
        self.arrived(self.R, 0)
        self.pair(2)
        self.start(self.A.at[2, pl.ds(0, 2)], self.T.at[0], 1, self.place.along_z(1))
        self.start(self.A.at[2, pl.ds(2, 2)], self.T.at[1], 2, self.place.along_z(-1))
        self.pair(1)
        self.pair(3)
        self.pair(0)

    def stage2(self):
        self.arrived(self.T.at[0], 1)
        self.A[1, 0:2] = (self.A[1, 0:2].astype(F32) + self.T[0].astype(F32)).astype(BF16)
        self.start(self.A.at[1], self.U.at[0], 3, self.place.along_z(1))
        self.arrived(self.T.at[1], 2)
        self.A[3, 2:4] = (self.A[3, 2:4].astype(F32) + self.T[1].astype(F32)).astype(BF16)
        self.start(self.A.at[3], self.U.at[1], 4, self.place.along_z(-1))

    def stage3(self):
        self.arrived(self.U.at[0], 3)
        self.arrived(self.U.at[1], 4)
        for d3 in range(4):
            total = self.A[0, d3].astype(F32) + self.U[0, d3].astype(F32)
            self.B[d3] = (total + self.U[1, d3].astype(F32)).astype(BF16)
        for d2 in (2, 1, 3):
            q = (self.place.y + d2) % 4
            self.start(self.B.at[:, q], self.Y.at[d2 - 1], 4 + d2, self.place.at(dy=d2))

    def stage4(self):
        for d2 in (1, 3, 2):
            self.arrived(self.Y.at[d2 - 1], 4 + d2)
        for d3 in range(4):
            total = self.B[d3, self.place.y].astype(F32) + self.Y[0, d3].astype(F32)
            total = total + self.Y[1, d3].astype(F32) + self.Y[2, d3].astype(F32)
            self.C[d3] = total.astype(BF16)
        low, high = self.low, self.high
        self.start(self.C.at[2, :, low], self.V.at[1, :, low], 8, self.place.along_x(2))
        self.start(self.C.at[2, :, high], self.V.at[1, :, high], 9, self.place.along_x(-2))
        self.start(self.C.at[1], self.V.at[0], 10, self.place.along_x(1))
        self.start(self.C.at[3], self.V.at[2], 11, self.place.along_x(-1))

    def stage5(self):
        self.arrived(self.V.at[0], 10)
        self.arrived(self.V.at[2], 11)
        self.arrived(self.V.at[1, :, self.low], 8)
        self.arrived(self.V.at[1, :, self.high], 9)
        total = self.C[0].astype(F32) + self.V[0].astype(F32)
        total = total + self.V[1].astype(F32) + self.V[2].astype(F32)
        self.E[0] = total.astype(BF16)
        self.start(self.E.at[0], self.Z, 12, self.place.partner())

    def stage6(self):
        self.arrived(self.Z, 12)
        self.E[1] = (self.E[0].astype(F32) + self.Z[...].astype(F32)).astype(BF16)
        for d2 in (2, 1, 3):
            self.start(self.E.at[1], self.O.at[self.place.y], 12 + d2, self.place.at(dy=d2))

    def stage7(self, write):
        for d2 in (1, 3, 2):
            self.arrived(self.O.at[(self.place.y - d2 + 4) % 4], 12 + d2)
        self.O[self.place.y] = self.E[1]
        for r in range(2):
            for k in range(2):
                write(r, k, self.O[2 * r + k].astype(F32))

    def drain(self):
        self.left(self.R, 0)
        self.left(self.T.at[0], 1)
        self.left(self.T.at[1], 2)
        self.left(self.U.at[0], 3)
        self.left(self.U.at[1], 4)
        for d2 in (1, 2, 3):
            self.left(self.Y.at[d2 - 1], 4 + d2)
            self.left(self.Z, 12 + d2)
        self.left(self.V.at[1, :, self.low], 8)
        self.left(self.V.at[1, :, self.high], 9)
        self.left(self.V.at[0], 10)
        self.left(self.V.at[2], 11)
        self.left(self.Z, 12)


SCRATCH = {
    "normed": ((384, 1024), F32),
    "inverse": ((384, 128), F32),
    "hidden": ((384, 1024), BF16),
    "hidden_t": ((1024, 384), BF16),
    "mcot": ((384, 1024), BF16),
    "live": ((384, 128), F32),
    "ga": ((4, 384, 256), BF16),
    "att": ((4, 384, 256), BF16),
    "qkv": ((384, 768), BF16),
    "dqkv": ((4, 384, 768), BF16),
    "bias": ((384, 384), F32),
    "gains": ((2, 1024), F32),
    "probs": ((2, 384, 384), BF16),
    "dscores": ((2, 384, 384), BF16),
    "gh": ((384, 1024), F32),
}


def prologue_tokens(S, tok_ref, count_ref, starts_ref):
    source = tok_ref[...].astype(F32)
    center = jnp.mean(source, axis=1, keepdims=True)
    centered = source - center
    variance = jnp.mean(centered * centered, axis=1, keepdims=True)
    inverse = lax.rsqrt(variance + 1e-06)
    S["normed"][...] = centered * inverse
    S["inverse"][...] = jnp.broadcast_to(inverse, (ROWS, 128))
    count = count_ref[0]
    down = lax.broadcasted_iota(jnp.int32, (ROWS, 1), 0)
    across = lax.broadcasted_iota(jnp.int32, (1, ROWS), 1)
    seg_down = jnp.zeros((ROWS, 1), jnp.int32)
    seg_across = jnp.zeros((1, ROWS), jnp.int32)
    for j in range(8):
        start = starts_ref[0, j]
        seg_down = seg_down + jnp.where(down >= start, 1, 0)
        seg_across = seg_across + jnp.where(across >= start, 1, 0)
    seg_down = jnp.where(down < count, seg_down, -1)
    seg_across = jnp.where(across < count, seg_across, -2)
    S["bias"][...] = jnp.where(seg_down == seg_across, 0.0, -1e30).astype(F32)
    alive = lax.broadcasted_iota(jnp.int32, (ROWS, 128), 0) < count
    S["live"][...] = jnp.where(alive, 1.0, 0.0).astype(F32)


def prologue_weights(S, tok_ref, cot_ref):
    weights = S["Wps"]
    small = weights[:, :, :, :, 1024:1152].reshape(1024, 128).astype(F32)
    S["gains"][...] = small.T[0:2, :]
    gain = S["gains"][0:1, :]
    shift = S["gains"][1:2, :]
    S["hidden"][...] = (S["normed"][...] * gain + shift).astype(BF16)
    S["hidden_t"][...] = S["hidden"][...].T
    cot = cot_ref[...]
    alive = S["live"][:, 0:1] > 0.5
    S["mcot"][...] = jnp.where(alive, cot.astype(F32), 0.0).astype(BF16)
    for g in range(4):
        part = weights[g, :, :, :, 0:1024].reshape(256, 1024)
        S["ga"][g] = nt(S["mcot"][...], part).astype(BF16)


def group(S, g, hook):
    weight = S["Wg"][g].reshape(1024, 768)
    for n in range(3):
        part = nn(S["hidden"][...], S["Wg"][g, :, :, :, :, n * 256 : n * 256 + 256].reshape(1024, 256))
        part = part.astype(BF16)
        S["qkv"][:, n * 256 : n * 256 + 256] = part * jnp.asarray(0.125, BF16) if n == 0 else part
    lane = lax.broadcasted_iota(jnp.int32, (ROWS, 128), 1)
    first = lane < 64
    for pair in range(2):
        q2 = S["qkv"][:, pair * 128 : pair * 128 + 128]
        k2 = S["qkv"][:, 256 + pair * 128 : 384 + pair * 128]
        v2 = S["qkv"][:, 512 + pair * 128 : 640 + pair * 128]
        o2 = S["ga"][g, :, pair * 128 : pair * 128 + 128]
        zero = jnp.zeros_like(q2)

        def own(a, h):
            return jnp.where(first, a, zero) if h == 0 else jnp.where(first, zero, a)

        for h in range(2):
            hook(2 * pair + h)
            scores = nt(own(q2, h), k2) + S["bias"][...]
            row_max = jnp.max(scores, axis=1, keepdims=True)
            expon = jnp.exp(scores - row_max)
            probs = expon * (1.0 / jnp.sum(expon, axis=1, keepdims=True))
            S["probs"][h] = probs.astype(BF16)
            grad_probs = nt(own(o2, h), v2)
            delta = jnp.sum(probs * grad_probs, axis=1, keepdims=True)
            S["dscores"][h] = (probs * (grad_probs - delta)).astype(BF16)
        att = sum(nn(S["probs"][h], own(v2, h)) for h in range(2))
        S["att"][g, :, pair * 128 : pair * 128 + 128] = att.astype(BF16)
        dv = sum(tn(S["probs"][h], own(o2, h)) for h in range(2))
        dq = sum(nn(S["dscores"][h], own(k2, h)) for h in range(2)) * 0.125
        dk = sum(tn(S["dscores"][h], own(q2, h)) for h in range(2))
        S["dqkv"][g, :, pair * 128 : pair * 128 + 128] = dq.astype(BF16)
        S["dqkv"][g, :, 256 + pair * 128 : 384 + pair * 128] = dk.astype(BF16)
        S["dqkv"][g, :, 512 + pair * 128 : 640 + pair * 128] = dv.astype(BF16)
    hook(4)
    for m in range(4):
        part = nn(S["hidden_t"][m * 256 : m * 256 + 256], S["dqkv"][g]).astype(BF16)
        part = part.reshape(4, 2, 2, 16, 768)
        for k in range(2):
            S["G"][g, m, :, :, :, k] = part[..., k * 384 : k * 384 + 384]
    hook(5)


def proj_grads(S):
    for g in range(4):
        part = tn(S["att"][g], S["mcot"][...]).astype(BF16).reshape(4, 2, 2, 16, 1024)
        for k in range(2):
            S["Gp"][g, :, :, :, k] = part[..., k * 512 : k * 512 + 512]


def grads_hidden(S, between):
    for n in range(4):
        S["gh"][:, n * 256 : n * 256 + 256] = sum(
            nt(S["dqkv"][g], S["Wg"][g, n].reshape(256, 768)) for g in range(4)
        )
        between(n)


def small_grads(S):
    gh = S["gh"][...]
    gain_term = jnp.sum(gh * S["normed"][...], axis=0, keepdims=True)
    shift_term = jnp.sum(gh, axis=0, keepdims=True)
    rows = lax.broadcasted_iota(jnp.int32, (128, 1024), 0)
    both = jnp.where(rows == 0, gain_term, jnp.where(rows == 1, shift_term, 0.0))
    columns = both.T.astype(BF16).reshape(4, 4, 2, 2, 16, 128)
    zero = jnp.zeros_like(columns)
    S["Gs"][:, :, :, :, 0, :, 0:128] = columns
    S["Gs"][:, :, :, :, 0, :, 128:256] = zero
    S["Gs"][:, :, :, :, 1, :, 0:128] = zero
    S["Gs"][:, :, :, :, 1, :, 128:256] = zero


def token_grads(S, cot_ref, out_ref):
    normed = S["normed"][...]
    grad_normed = S["gh"][...] * S["gains"][0:1, :]
    inner = grad_normed - jnp.mean(grad_normed, axis=1, keepdims=True)
    inner = inner - normed * jnp.mean(grad_normed * normed, axis=1, keepdims=True)
    out_ref[...] = (cot_ref[...].astype(F32) + S["inverse"][:, 0:1] * inner).astype(BF16)


COMM = {}
for _name, _shape in reduce_shapes(768).items():
    COMM["g_" + _name] = ((4,) + _shape, BF16)
for _name, _shape in reduce_shapes(1024).items():
    COMM["p_" + _name] = (_shape, BF16)
for _name, _shape in reduce_shapes(512).items():
    COMM["s_" + _name] = (_shape, BF16)
COMM["Wg"] = ((4, 4, 4, 2, 32, 768), BF16)
COMM["Wps"] = ((4, 4, 2, 32, 1152), BF16)
COMM["G"] = ((4, 4, 4, 2, 2, 2, 16, 384), BF16)
COMM["Gp"] = ((4, 4, 2, 2, 2, 16, 512), BF16)
COMM["Gs"] = ((4, 4, 2, 2, 2, 16, 256), BF16)


def kernel(
    scale,
    count_ref,
    starts_ref,
    tok_ref,
    cot_ref,
    qkv_ref,
    proj_ref,
    small_ref,
    out_ref,
    qkv_out,
    proj_out,
    small_out,
    *scratch,
):
    S = dict(zip(tuple(SCRATCH) + tuple(COMM), scratch))
    gs, gr, rs, rr, ls = scratch[len(S) :]
    place = Place()
    x, z, c = place.x, place.zlo, place.c

    local = []
    for n, (src, dst) in enumerate(
        [
            (proj_ref, S["Wps"].at[x, z, c, :, pl.ds(0, 1024)]),
            (small_ref, S["Wps"].at[x, z, c, :, pl.ds(1024, 128)]),
        ]
        + [
            (
                qkv_ref.at[:, pl.ds(part * 1024 + g * 256, 256)],
                S["Wg"].at[g, x, z, c, :, pl.ds(part * 256, 256)],
            )
            for g in range(4)
            for part in range(3)
        ]
    ):
        copy = pltpu.make_async_copy(src, dst, ls.at[n])
        copy.start()
        local.append(copy)

    def piece(k):
        if isinstance(k, int) and k == 0:
            return Gather(place, S["Wps"], gs.at[0], gr.at[0])
        return Gather(place, S["Wg"].at[k - 1], gs.at[k], gr.at[k])

    def term(k):
        buffers = [S["g_" + name].at[k] for name in REDUCE_NAMES]
        return Reduce(place, S["G"].at[k], buffers, 384, rs.at[k], rr.at[k])

    def write_group(g):
        def write(r, k, value):
            value = value * scale
            rows = pl.ds(r * 16, 16)

            def at(first, width):
                return pl.ds(pl.multiple_of(first + g * 256, 128), width)

            if k == 0:
                qkv_out[rows, at(0, 256)] = value[:, 0:256]
                qkv_out[rows, at(1024, 128)] = value[:, 256:384]
            else:
                qkv_out[rows, at(1152, 128)] = value[:, 0:128]
                qkv_out[rows, at(2048, 256)] = value[:, 128:384]

        return write

    def write_to(ref, half):
        def write(r, k, value):
            ref[r * 16 : r * 16 + 16, k * half : (k + 1) * half] = value * scale

        return write

    enter(place.all())
    for copy in local:
        copy.wait()
    for k in range(3):
        piece(k).stage0()
    prologue_tokens(S, tok_ref, count_ref, starts_ref)
    piece(0).stage1()
    piece(1).stage1()
    piece(0).stage2()
    piece(1).stage2()
    piece(2).stage1()
    piece(0).stage3()
    piece(3).stage0()
    piece(1).stage3()
    piece(2).stage2()
    piece(0).stage4()
    piece(1).stage4()
    piece(3).stage1()
    piece(0).stage5()
    prologue_weights(S, tok_ref, cot_ref)
    piece(2).stage3()
    piece(1).stage5()

    def body(g, carry):
        def hook(k):
            gathers = {
                0: ((2, "stage4"), (3, "stage2")),
                1: ((4, "stage0"),),
                2: ((3, "stage3"),),
                3: ((4, "stage1"),),
                4: ((2, "stage5"),),
            }
            for ahead, stage in gathers.get(k, ()):

                @pl.when(g + ahead <= 4)
                def _():
                    getattr(piece(g + ahead), stage)()

            reduces = {
                0: ((2, "stage4"),),
                1: ((1, "stage1"),),
                2: ((2, "stage5"),),
                3: ((1, "stage2"),),
                4: ((2, "stage6"),),
                5: ((1, "stage3"), (2, "stage7"), (0, "stage0")),
            }
            for behind, stage in reduces.get(k, ()):

                @pl.when(g >= behind)
                def _():
                    if stage == "stage7":
                        term(g - behind).stage7(write_group(g - behind))
                    else:
                        getattr(term(g - behind), stage)()

        group(S, g, hook)
        return carry

    lax.fori_loop(0, 4, body, 0)

    proj = Reduce(
        place, S["Gp"], [S["p_" + n] for n in REDUCE_NAMES], 512, rs.at[4], rr.at[4]
    )
    small = Reduce(
        place, S["Gs"], [S["s_" + n] for n in REDUCE_NAMES], 256, rs.at[5], rr.at[5]
    )
    proj_grads(S)
    proj.stage0()
    term(3).stage1()
    term(2).stage4()

    def between(n):
        if n == 0:
            proj.stage1()
        elif n == 1:
            term(3).stage2()
            term(2).stage5()
        elif n == 2:
            proj.stage2()
        else:
            term(3).stage3()

    grads_hidden(S, between)
    small_grads(S)
    small.stage0()
    term(2).stage6()
    proj.stage3()
    small.stage1()
    token_grads(S, cot_ref, out_ref)
    term(3).stage4()
    small.stage2()
    proj.stage4()
    term(3).stage5()
    small.stage3()
    term(2).stage7(write_group(2))
    proj.stage5()
    term(3).stage6()
    small.stage4()
    proj.stage6()
    small.stage5()
    term(3).stage7(write_group(3))
    small.stage6()
    proj.stage7(write_to(proj_out, 512))
    small.stage7(write_to(small_out, 256))

    piece(0).drain()

    def drain(k, carry):
        piece(k + 1).drain()
        term(k).drain()
        return carry

    lax.fori_loop(0, 4, drain, 0)
    proj.drain()
    small.drain()


def fused(counts, starts, tokens, cotangent, qkv_weight, proj_weight, small, scale):
    anyspace = pl.BlockSpec(memory_space=pl.ANY)
    vmem = pl.BlockSpec(memory_space=pltpu.VMEM)
    smem = pl.BlockSpec(memory_space=pltpu.SMEM)
    buffers = tuple(SCRATCH.values()) + tuple(COMM.values())
    return pl.pallas_call(
        functools.partial(kernel, scale),
        out_shape=[
            jax.ShapeDtypeStruct((ROWS, D), BF16),
            jax.ShapeDtypeStruct((32, 3072), F32),
            jax.ShapeDtypeStruct((32, 1024), F32),
            jax.ShapeDtypeStruct((32, 512), F32),
        ],
        in_specs=[smem, smem, vmem, vmem, anyspace, anyspace, anyspace],
        out_specs=[vmem] * 4,
        scratch_shapes=[pltpu.VMEM(*b) for b in buffers]
        + [
            pltpu.SemaphoreType.DMA((5, GATHER_SEMS)),
            pltpu.SemaphoreType.DMA((5, GATHER_SEMS)),
            pltpu.SemaphoreType.DMA((6, REDUCE_SEMS)),
            pltpu.SemaphoreType.DMA((6, REDUCE_SEMS)),
            pltpu.SemaphoreType.DMA((14,)),
        ],
        compiler_params=pltpu.CompilerParams(
            collective_id=0, has_side_effects=True, vmem_limit_bytes=63 * 2**20
        ),
        name="fused",
    )(counts, starts, tokens, cotangent, qkv_weight, proj_weight, small)


def per_device(
    tokens, cotangent, patch_count, image_starts, qkv_weight, proj_weight, norm_gain, norm_shift
):
    small = jnp.pad(jnp.stack([norm_gain, norm_shift], axis=1), ((0, 0), (0, 126)))
    everyone = lax.axis_size("dp") * lax.axis_size("fsdp")
    scale = 1.0 / math.sqrt(tokens.shape[0] * everyone)
    grad_block, qkv_grad, proj_grad, small_grad = fused(
        patch_count, image_starts, tokens, cotangent, qkv_weight, proj_weight, small, scale
    )
    return (grad_block, qkv_grad, proj_grad, small_grad[:, 0], small_grad[:, 1])


def solution(mesh):
    placed = (
        P(("dp", "fsdp"), None),
        P(("dp", "fsdp"), None),
        P(("dp", "fsdp")),
        P(("dp", "fsdp"), None),
        P("fsdp", None),
        P("fsdp", None),
        P("fsdp"),
        P("fsdp"),
    )
    return jax.shard_map(
        per_device,
        mesh=mesh,
        in_specs=placed,
        out_specs=(P(("dp", "fsdp"), None), P("fsdp", None), P("fsdp", None), P("fsdp"), P("fsdp")),
        check_vma=False,
    )
```

```python
import functools
import math

import jax
import jax.numpy as jnp
from jax import lax
from jax.experimental import pallas as pl
from jax.experimental.pallas import tpu as pltpu
from jax.sharding import PartitionSpec as P

MESH = pl.DeviceIdType.MESH
F32 = jnp.float32
BF16 = jnp.bfloat16
D = 1024
ROWS = 384


def nn(a, b):
    return lax.dot_general(a, b, (((1,), (0,)), ((), ())), preferred_element_type=F32)


def nt(a, b):
    return lax.dot_general(a, b, (((1,), (1,)), ((), ())), preferred_element_type=F32)


def tn(a, b):
    return lax.dot_general(a, b, (((0,), (0,)), ((), ())), preferred_element_type=F32)


class Place:
    def __init__(self):
        dp, fsdp = lax.axis_index("dp"), lax.axis_index("fsdp")
        self.y, self.zhi = dp // 2, dp % 2
        self.c = fsdp % 2
        chip = fsdp // 2
        self.x, self.zlo = chip // 4, chip % 4
        self.z = self.zhi * 4 + self.zlo

    def at(self, dx=0, dy=0, dz=0, flip=0):
        x = (self.x + dx + 4) % 4
        y = (self.y + dy + 4) % 4
        z = (self.z + dz + 8) % 8
        c = self.c + flip * (1 - 2 * self.c)
        return {"dp": y * 2 + z // 4, "fsdp": (x * 4 + z % 4) * 2 + c}

    def along_x(self, d):
        return self.at(dx=(1 - self.c) * d, dz=self.c * d)

    def along_z(self, d):
        return self.at(dx=self.c * d, dz=(1 - self.c) * d)

    def chip(self, i, j):
        x = (self.x + (1 - self.c) * i + self.c * j + 8) % 4
        z = (self.zlo + self.c * i + (1 - self.c) * j + 8) % 4
        return x, z

    def sibling(self):
        return self.at(flip=1)

    def first(self, d):
        return self.at(dx=self.c * d, dy=(1 - self.c) * d)

    def second(self, d):
        return self.at(dx=(1 - self.c) * d, dy=self.c * d)

    def quarter(self, d1, d2):
        x = (self.x + self.c * d1 + (1 - self.c) * d2) % 4
        y = (self.y + (1 - self.c) * d1 + self.c * d2) % 4
        return x, y

    def all(self):
        return (
            [self.sibling()]
            + [self.at(dx=d) for d in (1, 2, 3)]
            + [self.at(dy=d) for d in (1, 2, 3)]
            + [self.at(dz=d) for d in range(1, 8)]
        )


def enter(devices, meanwhile):
    barrier = pltpu.get_barrier_semaphore()
    for device in devices:
        pl.semaphore_signal(barrier, inc=1, device_id=device, device_id_type=MESH)
    meanwhile()
    pl.semaphore_wait(barrier, len(devices))


class Copies:
    def __init__(self, place, send_sems, recv_sems):
        self.place, self.send_sems, self.recv_sems = place, send_sems, recv_sems

    def copy(self, src, dst, n, device):
        return pltpu.make_async_remote_copy(
            src_ref=src,
            dst_ref=dst,
            send_sem=self.send_sems.at[n],
            recv_sem=self.recv_sems.at[n],
            device_id=device,
            device_id_type=MESH,
        )

    def start(self, src, dst, n, device):
        self.copy(src, dst, n, device).start()

    def arrived(self, ref, n):
        self.copy(ref, ref, n, self.place.sibling()).wait_recv()

    def left(self, ref, n):
        self.copy(ref, ref, n, self.place.sibling()).wait_send()


GATHER_SEMS = 36
ORDER = (0, -1, 1, 2)


class Gather(Copies):
    def __init__(self, place, buffer, send_sems, recv_sems):
        super().__init__(place, send_sems, recv_sems)
        self.buffer = buffer

    def block(self, i, j, half=None):
        x, z = self.place.chip(i, j)
        ref = self.buffer.at[x, z, self.place.c]
        return ref if half is None else ref.at[pl.ds(half * 16, 16)]

    def forward(self, ref, n, device):
        self.start(ref, ref, n, device)

    def to_second(self, i):
        self.forward(self.block(i, 0), 4 + 4 * (i % 4), self.place.along_z(1))
        self.forward(self.block(i, 0), 5 + 4 * (i % 4), self.place.along_z(-1))
        self.to_sibling(i, 0)

    def to_sibling(self, i, j):
        self.forward(self.block(i, j), 20 + 4 * (i % 4) + (j % 4), self.place.sibling())

    def stage0(self):
        self.forward(self.block(0, 0), 0, self.place.along_x(1))
        self.forward(self.block(0, 0), 1, self.place.along_x(-1))
        self.to_second(0)

    def stage1(self):
        self.arrived(self.block(-1, 0), 0)
        self.forward(self.block(-1, 0, 0), 2, self.place.along_x(1))
        self.arrived(self.block(1, 0), 1)
        self.forward(self.block(1, 0, 1), 3, self.place.along_x(-1))
        self.to_second(-1)
        self.to_second(1)

    def stage2(self):
        self.arrived(self.block(2, 0, 0), 2)
        self.arrived(self.block(2, 0, 1), 3)
        self.to_second(2)

    def stage3(self):
        for i in ORDER:
            k = i % 4
            self.arrived(self.block(i, -1), 4 + 4 * k)
            self.forward(self.block(i, -1, 0), 6 + 4 * k, self.place.along_z(1))
            self.to_sibling(i, -1)
            self.arrived(self.block(i, 1), 5 + 4 * k)
            self.forward(self.block(i, 1, 1), 7 + 4 * k, self.place.along_z(-1))
            self.to_sibling(i, 1)

    def stage4(self):
        for i in ORDER:
            k = i % 4
            self.arrived(self.block(i, 2, 0), 6 + 4 * k)
            self.arrived(self.block(i, 2, 1), 7 + 4 * k)
            self.to_sibling(i, 2)

    def stage5(self):
        for i in range(4):
            for j in range(4):
                x, z = self.place.chip(j, i)
                self.arrived(self.buffer.at[x, z, 1 - self.place.c], 20 + 4 * i + j)

    def drain(self):
        whole, half = self.block(0, 0), self.block(0, 0, 0)
        for n in range(GATHER_SEMS):
            self.left(half if n in (2, 3) or (n < 20 and n % 4 > 1) else whole, n)


REDUCE_SEMS = 21


def reduce_shapes(half):
    return dict(
        R=(4, 4, 4, 16, half),
        A=(4, 4, 4, 16, half),
        T=(2, 2, 4, 16, half),
        U=(2, 4, 4, 16, half),
        B=(4, 4, 16, half),
        Y=(3, 4, 16, half),
        C=(4, 16, half),
        V=(8, 16, half),
        E=(16, half),
        O=(4, 16, half),
    )


REDUCE_NAMES = tuple(reduce_shapes(128))


class Reduce(Copies):
    def __init__(self, place, term, buffers, send_sems, recv_sems):
        super().__init__(place, send_sems, recv_sems)
        self.term = term
        for name, ref in zip(REDUCE_NAMES, buffers):
            setattr(self, name, ref)

    def stage0(self):
        at = self.place

        @pl.when(at.c == 1)
        def _():
            for d1 in (2, 1, 3, 0):
                src = self.term.at[:, :, 0, (at.y + d1) % 4]
                self.start(src, self.R.at[d1], d1, at.sibling())

        @pl.when(at.c == 0)
        def _():
            for d1 in (2, 1, 3, 0):
                src = self.term.at[(at.x + d1) % 4, :, 1]
                self.start(src, self.R.at[d1], d1, at.sibling())

    def pair(self, d1):
        at = self.place
        self.arrived(self.R.at[d1], d1)
        for d2 in range(4):
            x, y = at.quarter(d1, d2)
            for z in range(4):
                m = (1 - at.c) * x + at.c * z
                n = (1 - at.c) * z + at.c * y
                both = self.term[x, z, at.c, y].astype(F32) + self.R[d1, m, n].astype(F32)
                self.A[d1, d2, z] = both.astype(BF16)

    def stage1(self):
        at = self.place
        self.pair(2)
        self.start(self.A.at[2, pl.ds(0, 2)], self.T.at[0], 4, at.first(1))
        self.start(self.A.at[2, pl.ds(2, 2)], self.T.at[1], 5, at.first(-1))
        self.pair(1)
        self.pair(3)
        self.pair(0)

    def stage2(self):
        at = self.place
        self.arrived(self.T.at[0], 4)
        self.A[1, 0:2] = (self.A[1, 0:2].astype(F32) + self.T[0].astype(F32)).astype(BF16)
        self.start(self.A.at[1], self.U.at[0], 6, at.first(1))
        self.arrived(self.T.at[1], 5)
        self.A[3, 2:4] = (self.A[3, 2:4].astype(F32) + self.T[1].astype(F32)).astype(BF16)
        self.start(self.A.at[3], self.U.at[1], 7, at.first(-1))

    def stage3(self):
        at = self.place
        self.arrived(self.U.at[0], 6)
        self.arrived(self.U.at[1], 7)
        for d2 in (2, 1, 3, 0):
            total = self.A[0, d2].astype(F32) + self.U[0, d2].astype(F32)
            self.B[d2] = (total + self.U[1, d2].astype(F32)).astype(BF16)
            if d2:
                self.start(self.B.at[d2], self.Y.at[d2 - 1], 7 + d2, at.second(d2))

    def stage4(self):
        at = self.place
        for d2 in (1, 3, 2):
            self.arrived(self.Y.at[d2 - 1], 7 + d2)
        total = self.B[0].astype(F32) + self.Y[0].astype(F32)
        total = total + self.Y[1].astype(F32) + self.Y[2].astype(F32)
        self.C[...] = total.astype(BF16)
        for d in (4, 3, 5, 2, 6, 1, 7):
            self.start(self.C.at[(at.zlo + d) % 4], self.V.at[at.z], 10 + d, at.at(dz=d))
        self.V[at.z] = self.C[at.zlo]

    def stage5(self):
        at = self.place
        for d in (1, 7, 2, 6, 3, 5, 4):
            self.arrived(self.V.at[(at.z + 8 - d) % 8], 10 + d)
        total = self.V[0].astype(F32)
        for z in range(1, 8):
            total = total + self.V[z].astype(F32)
        self.E[...] = total.astype(BF16)
        for d in (2, 1, 3):
            self.start(self.E, self.O.at[at.y], 17 + d, at.at(dy=d))

    def stage6(self, write):
        at = self.place
        for d in (1, 3, 2):
            self.arrived(self.O.at[(at.y - d + 4) % 4], 17 + d)
        self.O[at.y] = self.E[...]
        for r in range(2):
            for k in range(2):
                write(r, k, self.O[2 * r + k])

    def drain(self):
        for d1 in range(4):
            self.left(self.R.at[d1], d1)
        self.left(self.T.at[0], 4)
        self.left(self.T.at[1], 5)
        self.left(self.U.at[0], 6)
        self.left(self.U.at[1], 7)
        for d2 in (1, 2, 3):
            self.left(self.B.at[0], 7 + d2)
        for n in range(11, 21):
            self.left(self.E, n)


SMALL_SEMS = 14


class Small(Copies):
    def __init__(self, place, tile, slots, send_sems, recv_sems):
        super().__init__(place, send_sems, recv_sems)
        self.tile, self.slots = tile, slots

    def step(self, n):
        at = self.place
        size, mine, first = ((4, at.x, 0), (4, at.y, 3), (8, at.z, 6), (2, at.c, 13))[n]
        other = (
            lambda d: at.at(dx=d),
            lambda d: at.at(dy=d),
            lambda d: at.at(dz=d),
            lambda d: at.sibling(),
        )[n]
        return size, mine, first, other

    def send(self, n):
        size, mine, first, other = self.step(n)
        for d in range(1, size):
            self.start(self.tile.at[n], self.slots.at[n, mine], first + d - 1, other(d))

    def receive(self, n):
        size, mine, first, _ = self.step(n)
        for d in range(1, size):
            self.arrived(self.slots.at[n, (mine - d + size) % size], first + d - 1)
        self.slots[n, mine] = self.tile[n]
        total = self.slots[n, 0].astype(F32)
        for k in range(1, size):
            total = total + self.slots[n, k].astype(F32)
        return total

    def stage0(self):
        self.send(0)

    def stage1(self):
        self.tile[1] = self.receive(0).astype(BF16)
        self.send(1)

    def stage2(self):
        self.tile[2] = self.receive(1).astype(BF16)
        self.send(2)

    def stage3(self):
        self.tile[3] = self.receive(2).astype(BF16)
        self.send(3)

    def stage4(self, write):
        write(self.receive(3))

    def drain(self):
        for n in range(SMALL_SEMS):
            self.left(self.tile.at[0], n)


class Timeline:
    def __init__(self):
        self.now, self.live = 0.0, []

    def add(self, stages):
        work = [self.now, len(self.live), list(stages)]
        self.live.append(work)
        self.run(self.now)
        return work

    def step(self, work):
        call, latency = work[2].pop(0)
        call()
        work[0] = max(self.now, work[0]) + latency

    def run(self, until):
        while True:
            ready = [w for w in self.live if w[2] and w[0] <= until]
            if not ready:
                return
            self.step(min(ready, key=lambda w: (w[0], w[1])))

    def spend(self, time):
        self.now += time
        self.run(self.now)

    def finish(self, work):
        while work[2]:
            self.now = max(self.now, min(w[0] for w in self.live if w[2]))
            self.run(self.now)


SCRATCH = {
    "normed": ((384, 1024), F32),
    "inverse": ((384, 128), F32),
    "hidden": ((384, 1024), BF16),
    "hidden_t": ((1024, 384), BF16),
    "mcot": ((384, 1024), BF16),
    "live": ((384, 128), F32),
    "ga": ((4, 384, 256), BF16),
    "att": ((4, 384, 256), BF16),
    "qkv": ((2, 384, 768), BF16),
    "dqkv": ((384, 768), BF16),
    "bias": ((384, 384), F32),
    "gains": ((2, 1024), F32),
    "probs": ((2, 4, 384, 384), F32),
    "low": ((2, 384, 384), BF16),
    "dscores": ((2, 384, 384), BF16),
    "gh": ((384, 1024), F32),
    "own": ((128, 128), F32),
    "own_low": ((32, 128), BF16),
    "sums": ((16, 128), F32),
}


def own_small(S, gain_ref, shift_ref):
    S["own"][...] = jnp.zeros((128, 128), F32)
    S["own"][0:1, 0:32] = gain_ref[...].astype(F32)
    S["own"][1:2, 0:32] = shift_ref[...].astype(F32)
    S["own_low"][...] = S["own"][...].T[0:32].astype(BF16)


def prologue_tokens(S, tok_ref, cot_ref, count_ref, starts_ref):
    source = tok_ref[...].astype(F32)
    center = jnp.mean(source, axis=1, keepdims=True)
    centered = source - center
    variance = jnp.mean(centered * centered, axis=1, keepdims=True)
    inverse = lax.rsqrt(variance + 1e-06)
    S["normed"][...] = centered * inverse
    S["inverse"][...] = jnp.broadcast_to(inverse, (ROWS, 128))
    count = count_ref[0]
    down = lax.broadcasted_iota(jnp.int32, (ROWS, 1), 0)
    across = lax.broadcasted_iota(jnp.int32, (1, ROWS), 1)
    seg_down = jnp.zeros((ROWS, 1), jnp.int32)
    seg_across = jnp.zeros((1, ROWS), jnp.int32)
    for j in range(8):
        start = starts_ref[0, j]
        seg_down = seg_down + jnp.where(down >= start, 1, 0)
        seg_across = seg_across + jnp.where(across >= start, 1, 0)
    seg_down = jnp.where(down < count, seg_down, -1)
    seg_across = jnp.where(across < count, seg_across, -2)
    S["bias"][...] = jnp.where(seg_down == seg_across, 0.0, -1e30).astype(F32)
    alive = lax.broadcasted_iota(jnp.int32, (ROWS, 128), 0) < count
    S["live"][...] = jnp.where(alive, 1.0, 0.0).astype(F32)
    alive = S["live"][:, 0:1] > 0.5
    S["mcot"][...] = jnp.where(alive, cot_ref[...].astype(F32), 0.0).astype(BF16)


def prologue_hidden(S):
    small = S["Wps"][:, :, :, :, 1024:1152].reshape(1024, 128).astype(F32)
    S["gains"][...] = small.T[0:2, :]
    gain = S["gains"][0:1, :]
    shift = S["gains"][1:2, :]
    S["hidden"][...] = (S["normed"][...] * gain + shift).astype(BF16)
    S["hidden_t"][...] = S["hidden"][...].T


def grads_attended(S):
    for g in range(4):
        part = S["Wps"][g, :, :, :, 0:1024].reshape(256, 1024)
        S["ga"][g] = nt(S["mcot"][...], part).astype(BF16)


def own(a, h):
    first = lax.broadcasted_iota(jnp.int32, (ROWS, 128), 1) < 64
    zero = jnp.zeros_like(a)
    return jnp.where(first, a, zero) if h == 0 else jnp.where(first, zero, a)


def lanes(ref, pair, part):
    return ref[:, part * 256 + pair * 128 : part * 256 + pair * 128 + 128]


def forward(S, g, spend):
    qkv, slot = S["qkv"].at[g % 2], g % 2
    for n in range(3):
        weight = S["Wg"][g, :, :, :, :, n * 256 : n * 256 + 256].reshape(1024, 256)
        part = nn(S["hidden"][...], weight).astype(BF16)
        qkv[:, n * 256 : n * 256 + 256] = part * jnp.asarray(0.125, BF16) if n == 0 else part
    spend(0.9)
    for pair in range(2):
        q2, k2, v2 = (lanes(qkv, pair, n) for n in range(3))
        for h in range(2):
            scores = nt(own(q2, h), k2) + S["bias"][...]
            row_max = jnp.max(scores, axis=1, keepdims=True)
            expon = jnp.exp(scores - row_max)
            probs = expon * (1.0 / jnp.sum(expon, axis=1, keepdims=True))
            S["probs"][slot, 2 * pair + h] = probs
            S["low"][h] = probs.astype(BF16)
        att = sum(nn(S["low"][h], own(v2, h)) for h in range(2))
        S["att"][g, :, pair * 128 : pair * 128 + 128] = att.astype(BF16)
        spend(1.0)


def backward(S, g, spend):
    qkv, slot = S["qkv"].at[g % 2], g % 2
    for pair in range(2):
        q2, k2, v2 = (lanes(qkv, pair, n) for n in range(3))
        o2 = S["ga"][g, :, pair * 128 : pair * 128 + 128]
        for h in range(2):
            probs = S["probs"][slot, 2 * pair + h]
            grad_probs = nt(own(o2, h), v2)
            delta = jnp.sum(probs * grad_probs, axis=1, keepdims=True)
            S["dscores"][h] = (probs * (grad_probs - delta)).astype(BF16)
            S["low"][h] = probs.astype(BF16)
        spend(0.8)
        dv = sum(tn(S["low"][h], own(o2, h)) for h in range(2))
        dq = sum(nn(S["dscores"][h], own(k2, h)) for h in range(2)) * 0.125
        dk = sum(tn(S["dscores"][h], own(q2, h)) for h in range(2))
        for n, part in enumerate((dq, dk, dv)):
            start = n * 256 + pair * 128
            S["dqkv"][:, start : start + 128] = part.astype(BF16)
        spend(0.8)


def weight_grads(S, g):
    for m in range(4):
        part = nn(S["hidden_t"][m * 256 : m * 256 + 256], S["dqkv"][...]).astype(BF16)
        part = part.reshape(4, 2, 2, 16, 768)
        for r in range(2):
            for k in range(2):
                S["G"][g, m, :, :, 2 * r + k] = part[:, :, r, :, k * 384 : k * 384 + 384]


def hidden_grads(S, g):
    for n in range(4):
        part = nt(S["dqkv"][...], S["Wg"][g, n].reshape(256, 768))
        columns = slice(n * 256, n * 256 + 256)
        S["gh"][:, columns] = part if g == 0 else S["gh"][:, columns] + part


def proj_grads(S):
    for g in range(4):
        part = tn(S["att"][g], S["mcot"][...]).astype(BF16).reshape(4, 2, 2, 16, 1024)
        for r in range(2):
            for k in range(2):
                S["Gp"][g, :, :, 2 * r + k] = part[:, :, r, :, k * 512 : k * 512 + 512]


def small_grads(S):
    gh = S["gh"][...]
    gain_term = jnp.sum(gh * S["normed"][...], axis=0, keepdims=True)
    shift_term = jnp.sum(gh, axis=0, keepdims=True)
    for r in range(8):
        S["sums"][r : r + 1, :] = gain_term[:, r * 128 : r * 128 + 128]
        S["sums"][8 + r : 9 + r, :] = shift_term[:, r * 128 : r * 128 + 128]
    S["tile"][0] = S["sums"][...].astype(BF16)


def token_grads(S):
    normed = S["normed"][...]
    grad_normed = S["gh"][...] * S["gains"][0:1, :]
    inner = grad_normed - jnp.mean(grad_normed, axis=1, keepdims=True)
    inner = inner - normed * jnp.mean(grad_normed * normed, axis=1, keepdims=True)
    S["gh"][...] = S["inverse"][:, 0:1] * inner


COMM = {}
for _name, _shape in reduce_shapes(384).items():
    COMM["g_" + _name] = ((4,) + _shape, BF16)
for _name, _shape in reduce_shapes(512).items():
    COMM["p_" + _name] = (_shape, BF16)
COMM["Wg"] = ((4, 4, 4, 2, 32, 768), BF16)
COMM["Wps"] = ((4, 4, 2, 32, 1152), BF16)
COMM["G"] = ((4, 4, 4, 2, 4, 16, 384), BF16)
COMM["Gp"] = ((4, 4, 2, 4, 16, 512), BF16)
COMM["tile"] = ((4, 16, 128), BF16)
COMM["slots"] = ((4, 8, 16, 128), BF16)


def kernel(
    count_ref,
    starts_ref,
    tok_ref,
    cot_ref,
    qkv_ref,
    proj_ref,
    gain_ref,
    shift_ref,
    out_ref,
    qkv_out,
    proj_out,
    gain_out,
    shift_out,
    *scratch,
):
    S = dict(zip(tuple(SCRATCH) + tuple(COMM), scratch))
    gs, gr, rs, rr, ss, sr, ls = scratch[len(S) :]
    place = Place()
    x, z, c = place.x, place.zlo, place.c
    time = Timeline()

    own_small(S, gain_ref, shift_ref)
    local = []
    for n, (src, dst) in enumerate(
        [
            (proj_ref, S["Wps"].at[x, z, c, :, pl.ds(0, 1024)]),
            (S["own_low"], S["Wps"].at[x, z, c, :, pl.ds(1024, 128)]),
        ]
        + [
            (
                qkv_ref.at[:, pl.ds(part * 1024 + g * 256, 256)],
                S["Wg"].at[g, x, z, c, :, pl.ds(part * 256, 256)],
            )
            for g in range(4)
            for part in range(3)
        ]
    ):
        copy = pltpu.make_async_copy(src, dst, ls.at[n])
        copy.start()
        local.append(copy)

    enter(place.all(), lambda: prologue_tokens(S, tok_ref, cot_ref, count_ref, starts_ref))
    for copy in local:
        copy.wait()

    buffers = [S["Wps"]] + [S["Wg"].at[g] for g in range(4)]
    gathers = [Gather(place, b, gs.at[k], gr.at[k]) for k, b in enumerate(buffers)]

    def gather(k):
        piece = gathers[k]
        calls = (piece.stage0, piece.stage1, piece.stage2, piece.stage3, piece.stage4, piece.stage5)
        return time.add(zip(calls, GATHER_TIMES))

    def write_group(g):
        def write(r, k, value):
            rows = slice(r * 16, r * 16 + 16)
            if k == 0:
                qkv_out[rows, g * 256 : g * 256 + 256] = value[:, 0:256]
                qkv_out[rows, 1024 + g * 256 : 1152 + g * 256] = value[:, 256:384]
            else:
                qkv_out[rows, 1152 + g * 256 : 1280 + g * 256] = value[:, 0:128]
                qkv_out[rows, 2048 + g * 256 : 2304 + g * 256] = value[:, 128:384]

        return write

    def write_proj(r, k, value):
        proj_out[r * 16 : r * 16 + 16, k * 512 : k * 512 + 512] = value

    def write_small(total):
        S["sums"][...] = total
        place_in_row = place.zlo * 2 + place.c
        for first, out in ((0, gain_out), (8, shift_out)):
            row = S["sums"][pl.ds(first + place.x * 2 + place.zlo // 2, 1), :]
            value = jnp.zeros((1, 32), F32)
            for k in range(4):
                value = jnp.where(place_in_row % 4 == k, row[:, k * 32 : k * 32 + 32], value)
            out[...] = value

    reduces = []

    def reduce(term, names, sem, write):
        piece = Reduce(place, term, names, rs.at[sem], rr.at[sem])
        reduces.append(piece)
        calls = (piece.stage0, piece.stage1, piece.stage2, piece.stage3, piece.stage4)
        calls += (piece.stage5, functools.partial(piece.stage6, write))
        return time.add(zip(calls, REDUCE_TIMES))

    works = []
    for k in GATHER_ORDER:
        works.append((k, gather(k)))
        time.now += GATHER_GAP
    works = [w for _, w in sorted(works, key=lambda pair: pair[0])]
    time.now = 0.0
    time.finish(works[0])
    prologue_hidden(S)
    time.spend(1.0)
    time.finish(works[1])
    forward(S, 0, time.spend)
    grads_attended(S)
    time.spend(1.0)
    for g in range(4):
        if g < 3:
            time.finish(works[g + 2])
            forward(S, g + 1, time.spend)
            if g == 2:
                proj_grads(S)
                reduce(S["Gp"], [S["p_" + n] for n in REDUCE_NAMES], 4, write_proj)
        backward(S, g, time.spend)
        weight_grads(S, g)
        names = [S["g_" + n].at[g] for n in REDUCE_NAMES]
        reduce(S["G"].at[g], names, g, write_group(g))
        time.spend(0.8)
        hidden_grads(S, g)
        time.spend(1.0)
    small_grads(S)
    small = Small(place, S["tile"], S["slots"], ss, sr)
    calls = (small.stage0, small.stage1, small.stage2, small.stage3)
    calls += (functools.partial(small.stage4, write_small),)
    time.add(zip(calls, SMALL_TIMES))
    token_grads(S)
    out = pltpu.make_async_copy(S["gh"], out_ref, ls.at[0])
    out.start()
    time.spend(0.8)
    for work in list(time.live):
        time.finish(work)
    out.wait()
    for piece in gathers + reduces + [small]:
        piece.drain()


GATHER_ORDER = (0, 1, 2, 3, 4)
GATHER_GAP = 3.0
GATHER_TIMES = (3.0, 3.0, 3.0, 4.0, 2.5, 0.0)
REDUCE_TIMES = (2.5, 3.0, 4.0, 3.5, 4.0, 3.0, 0.0)
SMALL_TIMES = (2.5, 2.5, 4.0, 1.5, 0.0)


def fused(counts, starts, tokens, cotangent, qkv_weight, proj_weight, gain, shift):
    anyspace = pl.BlockSpec(memory_space=pl.ANY)
    vmem = pl.BlockSpec(memory_space=pltpu.VMEM)
    smem = pl.BlockSpec(memory_space=pltpu.SMEM)
    buffers = tuple(SCRATCH.values()) + tuple(COMM.values())
    return pl.pallas_call(
        kernel,
        out_shape=[
            jax.ShapeDtypeStruct((ROWS, D), F32),
            jax.ShapeDtypeStruct((32, 3072), BF16),
            jax.ShapeDtypeStruct((32, 1024), BF16),
            jax.ShapeDtypeStruct((1, 32), F32),
            jax.ShapeDtypeStruct((1, 32), F32),
        ],
        in_specs=[smem, smem, vmem, vmem, anyspace, anyspace, vmem, vmem],
        out_specs=[anyspace] + [vmem] * 4,
        scratch_shapes=[pltpu.VMEM(*b) for b in buffers]
        + [
            pltpu.SemaphoreType.DMA((5, GATHER_SEMS)),
            pltpu.SemaphoreType.DMA((5, GATHER_SEMS)),
            pltpu.SemaphoreType.DMA((5, REDUCE_SEMS)),
            pltpu.SemaphoreType.DMA((5, REDUCE_SEMS)),
            pltpu.SemaphoreType.DMA((SMALL_SEMS,)),
            pltpu.SemaphoreType.DMA((SMALL_SEMS,)),
            pltpu.SemaphoreType.DMA((14,)),
        ],
        compiler_params=pltpu.CompilerParams(
            collective_id=0, has_side_effects=True, vmem_limit_bytes=67043328
        ),
        name="fused",
    )(counts, starts, tokens, cotangent, qkv_weight, proj_weight, gain, shift)


def per_device(
    tokens, cotangent, patch_count, image_starts, qkv_weight, proj_weight, norm_gain, norm_shift
):
    everyone = lax.axis_size("dp") * lax.axis_size("fsdp")
    scale = 1.0 / math.sqrt(tokens.shape[0] * everyone)
    through_norm, qkv_grad, proj_grad, gain_grad, shift_grad = fused(
        patch_count,
        image_starts,
        tokens,
        cotangent,
        qkv_weight,
        proj_weight,
        norm_gain.reshape(1, -1),
        norm_shift.reshape(1, -1),
    )
    return (
        (cotangent.astype(F32) + through_norm).astype(BF16),
        qkv_grad.astype(F32) * scale,
        proj_grad.astype(F32) * scale,
        gain_grad.reshape(-1) * scale,
        shift_grad.reshape(-1) * scale,
    )


def solution(mesh):
    placed = (
        P(("dp", "fsdp"), None),
        P(("dp", "fsdp"), None),
        P(("dp", "fsdp")),
        P(("dp", "fsdp"), None),
        P("fsdp", None),
        P("fsdp", None),
        P("fsdp"),
        P("fsdp"),
    )
    return jax.shard_map(
        per_device,
        mesh=mesh,
        in_specs=placed,
        out_specs=(P(("dp", "fsdp"), None), P("fsdp", None), P("fsdp", None), P("fsdp"), P("fsdp")),
        check_vma=False,
    )
```

```python
import functools
import math

import jax
import jax.numpy as jnp
from jax import lax
from jax.experimental import pallas as pl
from jax.experimental.pallas import tpu as pltpu
from jax.sharding import PartitionSpec as P

MESH = pl.DeviceIdType.MESH
F32 = jnp.float32
BF16 = jnp.bfloat16
D = 1024
ROWS = 384


def nn(a, b):
    return lax.dot_general(a, b, (((1,), (0,)), ((), ())), preferred_element_type=F32)


def nt(a, b):
    return lax.dot_general(a, b, (((1,), (1,)), ((), ())), preferred_element_type=F32)


def tn(a, b):
    return lax.dot_general(a, b, (((0,), (0,)), ((), ())), preferred_element_type=F32)


class Place:
    def __init__(self):
        dp, fsdp = lax.axis_index("dp"), lax.axis_index("fsdp")
        self.y, self.zhi = dp // 2, dp % 2
        self.c = fsdp % 2
        chip = fsdp // 2
        self.x, self.zlo = chip // 4, chip % 4
        self.z = self.zhi * 4 + self.zlo

    def at(self, dx=0, dy=0, dz=0, flip=0):
        x = (self.x + dx + 4) % 4
        y = (self.y + dy + 4) % 4
        z = (self.z + dz + 8) % 8
        c = self.c + flip * (1 - 2 * self.c)
        return {"dp": y * 2 + z // 4, "fsdp": (x * 4 + z % 4) * 2 + c}

    def along_x(self, d):
        return self.at(dx=(1 - self.c) * d, dz=self.c * d)

    def along_z(self, d):
        return self.at(dx=self.c * d, dz=(1 - self.c) * d)

    def chip(self, i, j):
        x = (self.x + (1 - self.c) * i + self.c * j + 8) % 4
        z = (self.zlo + self.c * i + (1 - self.c) * j + 8) % 4
        return x, z

    def sibling(self):
        return self.at(flip=1)

    def first(self, d):
        return self.at(dx=self.c * d, dy=(1 - self.c) * d)

    def second(self, d):
        return self.at(dx=(1 - self.c) * d, dy=self.c * d)

    def quarter(self, d1, d2):
        x = (self.x + self.c * d1 + (1 - self.c) * d2) % 4
        y = (self.y + (1 - self.c) * d1 + self.c * d2) % 4
        return x, y

    def all(self):
        return (
            [self.sibling()]
            + [self.at(dx=d) for d in (1, 2, 3)]
            + [self.at(dy=d) for d in (1, 2, 3)]
            + [self.at(dz=d) for d in range(1, 8)]
        )


def enter(devices, meanwhile):
    barrier = pltpu.get_barrier_semaphore()
    for device in devices:
        pl.semaphore_signal(barrier, inc=1, device_id=device, device_id_type=MESH)
    meanwhile()
    pl.semaphore_wait(barrier, len(devices))


class Copies:
    def __init__(self, place, send_sems, recv_sems):
        self.place, self.send_sems, self.recv_sems = place, send_sems, recv_sems

    def copy(self, src, dst, out, into, device):
        return pltpu.make_async_remote_copy(
            src_ref=src,
            dst_ref=dst,
            send_sem=self.send_sems.at[out],
            recv_sem=self.recv_sems.at[into],
            device_id=device,
            device_id_type=MESH,
        )

    def start(self, src, dst, out, into, device):
        self.copy(src, dst, out, into, device).start()

    def arrived(self, ref, into):
        self.copy(ref, ref, 0, into, self.place.sibling()).wait_recv()

    def left(self, ref, out):
        self.copy(ref, ref, out, 0, self.place.sibling()).wait_send()


GATHER_SEMS = (3, 13)
ORDER = (0, -1, 1, 2)


class Gather(Copies):
    def __init__(self, place, buffer, direct, send_sems, recv_sems):
        super().__init__(place, send_sems, recv_sems)
        self.buffer, self.direct = buffer, direct

    def block(self, i, j, half=None):
        x, z = self.place.chip(i, j)
        ref = self.buffer.at[x, z, self.place.c]
        return ref if half is None else ref.at[pl.ds(half * 16, 16)]

    def forward(self, ref, out, into, device):
        self.start(ref, ref, out, into, device)

    def to_second(self, i):
        k = 3 + 2 * (i % 4)
        self.forward(self.block(i, 0), 1, k, self.place.along_z(1))
        self.forward(self.block(i, 0), 1, k + 1, self.place.along_z(-1))
        if self.direct:
            self.forward(self.block(i, 0, 0), 1, 11, self.place.along_z(2))
            self.forward(self.block(i, 0, 1), 1, 11, self.place.along_z(-2))
        self.to_sibling(i, 0)

    def to_sibling(self, i, j):
        self.forward(self.block(i, j), 2, 12, self.place.sibling())

    def stage0(self):
        self.forward(self.block(0, 0), 0, 0, self.place.along_x(1))
        self.forward(self.block(0, 0), 0, 1, self.place.along_x(-1))
        self.forward(self.block(0, 0, 0), 0, 2, self.place.along_x(2))
        self.forward(self.block(0, 0, 1), 0, 2, self.place.along_x(-2))
        self.to_second(0)

    def stage1(self):
        self.arrived(self.block(-1, 0), 0)
        self.to_second(-1)
        self.arrived(self.block(1, 0), 1)
        self.to_second(1)

    def stage2(self):
        self.arrived(self.block(2, 0), 2)
        self.to_second(2)

    def stage3(self):
        for i in ORDER:
            k = 3 + 2 * (i % 4)
            self.arrived(self.block(i, -1), k)
            if not self.direct:
                self.forward(self.block(i, -1, 0), 1, 11, self.place.along_z(1))
            self.to_sibling(i, -1)
            self.arrived(self.block(i, 1), k + 1)
            if not self.direct:
                self.forward(self.block(i, 1, 1), 1, 11, self.place.along_z(-1))
            self.to_sibling(i, 1)

    def stage4(self):
        self.arrived(self.buffer.at[0, :, 0], 11)
        for i in ORDER:
            self.to_sibling(i, 2)

    def stage5(self):
        self.arrived(self.buffer.at[:, :, 1 - self.place.c], 12)

    def drain(self):
        self.left(self.buffer.at[0, pl.ds(0, 3), 0], 0)
        self.left(self.buffer.at[pl.ds(0, 3), :, 0], 1)
        self.left(self.buffer.at[:, :, 0], 2)


REDUCE_SEMS = (5, 8)


def reduce_shapes(half):
    return dict(
        R=(4, 4, 4, 16, half),
        A=(4, 4, 4, 16, half),
        T=(2, 2, 4, 16, half),
        U=(2, 4, 4, 16, half),
        B=(4, 4, 16, half),
        Y=(3, 4, 16, half),
        C=(4, 16, half),
        V=(8, 16, half),
        E=(16, half),
        O=(4, 16, half),
    )


REDUCE_NAMES = tuple(reduce_shapes(128))


class Reduce(Copies):
    def __init__(self, place, term, buffers, send_sems, recv_sems):
        super().__init__(place, send_sems, recv_sems)
        self.term = term
        for name, ref in zip(REDUCE_NAMES, buffers):
            setattr(self, name, ref)

    def stage0(self):
        at = self.place

        @pl.when(at.c == 1)
        def _():
            for d1 in (2, 1, 3, 0):
                src = self.term.at[:, :, 0, (at.y + d1) % 4]
                self.start(src, self.R.at[d1], 0, 0 if d1 == 2 else 1, at.sibling())

        @pl.when(at.c == 0)
        def _():
            for d1 in (2, 1, 3, 0):
                src = self.term.at[(at.x + d1) % 4, :, 1]
                self.start(src, self.R.at[d1], 0, 0 if d1 == 2 else 1, at.sibling())

    def pair(self, d1):
        at = self.place
        for d2 in range(4):
            x, y = at.quarter(d1, d2)
            for z in range(4):
                m = (1 - at.c) * x + at.c * z
                n = (1 - at.c) * z + at.c * y
                both = self.term[x, z, at.c, y].astype(F32) + self.R[d1, m, n].astype(F32)
                self.A[d1, d2, z] = both.astype(BF16)

    def stage1(self):
        at = self.place
        self.arrived(self.R.at[2], 0)
        self.pair(2)
        self.start(self.A.at[2, pl.ds(0, 2)], self.T.at[0], 1, 2, at.first(1))
        self.start(self.A.at[2, pl.ds(2, 2)], self.T.at[1], 1, 3, at.first(-1))
        self.arrived(self.R.at[pl.ds(0, 3)], 1)
        self.pair(1)
        self.pair(3)
        self.pair(0)

    def stage2(self):
        at = self.place
        self.arrived(self.T.at[0], 2)
        self.A[1, 0:2] = (self.A[1, 0:2].astype(F32) + self.T[0].astype(F32)).astype(BF16)
        self.start(self.A.at[1], self.U.at[0], 1, 4, at.first(1))
        self.arrived(self.T.at[1], 3)
        self.A[3, 2:4] = (self.A[3, 2:4].astype(F32) + self.T[1].astype(F32)).astype(BF16)
        self.start(self.A.at[3], self.U.at[1], 1, 4, at.first(-1))

    def stage3(self):
        at = self.place
        self.arrived(self.U, 4)
        for d2 in (2, 1, 3, 0):
            total = self.A[0, d2].astype(F32) + self.U[0, d2].astype(F32)
            self.B[d2] = (total + self.U[1, d2].astype(F32)).astype(BF16)
            if d2:
                self.start(self.B.at[d2], self.Y.at[d2 - 1], 2, 5, at.second(d2))

    def stage4(self):
        at = self.place
        self.arrived(self.Y, 5)
        total = self.B[0].astype(F32) + self.Y[0].astype(F32)
        total = total + self.Y[1].astype(F32) + self.Y[2].astype(F32)
        self.C[...] = total.astype(BF16)
        for d in (4, 3, 5, 2, 6, 1, 7):
            self.start(self.C.at[(at.zlo + d) % 4], self.V.at[at.z], 3, 6, at.at(dz=d))
        self.V[at.z] = self.C[at.zlo]

    def stage5(self):
        at = self.place
        self.arrived(self.V.at[pl.ds(0, 7)], 6)
        total = self.V[0].astype(F32)
        for z in range(1, 8):
            total = total + self.V[z].astype(F32)
        self.E[...] = total.astype(BF16)
        for d in (2, 1, 3):
            self.start(self.E, self.O.at[at.y], 4, 7, at.at(dy=d))

    def stage6(self, write):
        at = self.place
        self.arrived(self.O.at[pl.ds(0, 3)], 7)
        self.O[at.y] = self.E[...]
        for r in range(2):
            for k in range(2):
                write(r, k, self.O[2 * r + k])

    def drain(self):
        self.left(self.R, 0)
        self.left(self.A.at[pl.ds(0, 3)], 1)
        self.left(self.A.at[0, pl.ds(0, 3)], 2)
        self.left(self.V.at[pl.ds(0, 7)], 3)
        self.left(self.O.at[pl.ds(0, 3)], 4)


SMALL_SEMS = (4, 4)


class Small(Copies):
    def __init__(self, place, tile, slots, send_sems, recv_sems):
        super().__init__(place, send_sems, recv_sems)
        self.tile, self.slots = tile, slots

    def step(self, n):
        at = self.place
        size, mine = ((4, at.x), (4, at.y), (8, at.z), (2, at.c))[n]
        other = (
            lambda d: at.at(dx=d),
            lambda d: at.at(dy=d),
            lambda d: at.at(dz=d),
            lambda d: at.sibling(),
        )[n]
        return size, mine, other

    def send(self, n):
        size, mine, other = self.step(n)
        for d in range(1, size):
            self.start(self.tile.at[n], self.slots.at[n, mine], n, n, other(d))

    def receive(self, n):
        size, mine, _ = self.step(n)
        self.arrived(self.slots.at[n, pl.ds(0, size - 1)], n)
        self.slots[n, mine] = self.tile[n]
        total = self.slots[n, 0].astype(F32)
        for k in range(1, size):
            total = total + self.slots[n, k].astype(F32)
        return total

    def stage0(self):
        self.send(0)

    def stage1(self):
        self.tile[1] = self.receive(0).astype(BF16)
        self.send(1)

    def stage2(self):
        self.tile[2] = self.receive(1).astype(BF16)
        self.send(2)

    def stage3(self):
        self.tile[3] = self.receive(2).astype(BF16)
        self.send(3)

    def stage4(self, write):
        write(self.receive(3))

    def drain(self):
        for n in range(4):
            self.left(self.slots.at[n, pl.ds(0, self.step(n)[0] - 1)], n)


class Timeline:
    def __init__(self):
        self.now, self.live = 0.0, []

    def add(self, stages, start=0.0, first=0.0):
        work = [max(start, self.now), first, len(self.live), list(stages)]
        self.live.append(work)
        self.run(self.now)
        return work

    def step(self, work):
        call, latency = work[3].pop(0)
        call()
        work[0] = max(self.now, work[0]) + latency

    def run(self, until):
        while True:
            ready = [w for w in self.live if w[3] and w[0] <= until]
            if not ready:
                return
            self.step(min(ready, key=lambda w: (w[0] - w[1], w[2])))

    def spend(self, time):
        self.now += time
        self.run(self.now)

    def finish(self, work):
        while work[3]:
            self.now = max(self.now, min(w[0] for w in self.live if w[3]))
            self.run(self.now)


SCRATCH = {
    "normed": ((384, 1024), F32),
    "inverse": ((384, 128), F32),
    "hidden": ((384, 1024), BF16),
    "hidden_t": ((1024, 384), BF16),
    "mcot": ((384, 1024), BF16),
    "live": ((384, 128), F32),
    "ga": ((4, 384, 256), BF16),
    "att": ((4, 384, 256), BF16),
    "qkv": ((2, 384, 768), BF16),
    "dqkv": ((384, 768), BF16),
    "bias": ((384, 384), F32),
    "gains": ((2, 1024), F32),
    "probs": ((2, 4, 384, 384), F32),
    "low": ((2, 384, 384), BF16),
    "dscores": ((2, 384, 384), BF16),
    "gh": ((384, 1024), F32),
    "tokens": ((384, 1024), BF16),
    "cot": ((384, 1024), BF16),
    "own": ((128, 128), F32),
    "own_low": ((32, 128), BF16),
    "sums": ((16, 128), F32),
}


def own_small(S, gain_ref, shift_ref):
    S["own"][...] = jnp.zeros((128, 128), F32)
    S["own"][0:1, 0:32] = gain_ref[...].astype(F32)
    S["own"][1:2, 0:32] = shift_ref[...].astype(F32)
    S["own_low"][...] = S["own"][...].T[0:32].astype(BF16)


def prologue_tokens(S, count_ref, starts_ref):
    source = S["tokens"][...].astype(F32)
    center = jnp.mean(source, axis=1, keepdims=True)
    centered = source - center
    variance = jnp.mean(centered * centered, axis=1, keepdims=True)
    inverse = lax.rsqrt(variance + 1e-06)
    S["normed"][...] = centered * inverse
    S["inverse"][...] = jnp.broadcast_to(inverse, (ROWS, 128))
    count = count_ref[0]
    down = lax.broadcasted_iota(jnp.int32, (ROWS, 1), 0)
    across = lax.broadcasted_iota(jnp.int32, (1, ROWS), 1)
    seg_down = jnp.zeros((ROWS, 1), jnp.int32)
    seg_across = jnp.zeros((1, ROWS), jnp.int32)
    for j in range(8):
        start = starts_ref[0, j]
        seg_down = seg_down + jnp.where(down >= start, 1, 0)
        seg_across = seg_across + jnp.where(across >= start, 1, 0)
    seg_down = jnp.where(down < count, seg_down, -1)
    seg_across = jnp.where(across < count, seg_across, -2)
    S["bias"][...] = jnp.where(seg_down == seg_across, 0.0, -1e30).astype(F32)
    alive = lax.broadcasted_iota(jnp.int32, (ROWS, 128), 0) < count
    S["live"][...] = jnp.where(alive, 1.0, 0.0).astype(F32)
    alive = S["live"][:, 0:1] > 0.5
    S["mcot"][...] = jnp.where(alive, S["cot"][...].astype(F32), 0.0).astype(BF16)


def prologue_hidden(S):
    small = S["W0"][:, :, :, :, 768:896].reshape(1024, 128).astype(F32)
    S["gains"][...] = small.T[0:2, :]
    gain = S["gains"][0:1, :]
    shift = S["gains"][1:2, :]
    S["hidden"][...] = (S["normed"][...] * gain + shift).astype(BF16)
    S["hidden_t"][...] = S["hidden"][...].T


def grads_attended(S):
    for g in range(4):
        part = S["Wp"][g].reshape(256, 1024)
        S["ga"][g] = nt(S["mcot"][...], part).astype(BF16)


def own(a, h):
    first = lax.broadcasted_iota(jnp.int32, (ROWS, 128), 1) < 64
    zero = jnp.zeros_like(a)
    return jnp.where(first, a, zero) if h == 0 else jnp.where(first, zero, a)


def lanes(ref, pair, part):
    return ref[:, part * 256 + pair * 128 : part * 256 + pair * 128 + 128]


def forward(S, g, spend):
    qkv, slot = S["qkv"].at[g % 2], g % 2
    for n in range(3):
        weight = S[f"W{g}"][:, :, :, :, n * 256 : n * 256 + 256].reshape(1024, 256)
        part = nn(S["hidden"][...], weight).astype(BF16)
        qkv[:, n * 256 : n * 256 + 256] = part * jnp.asarray(0.125, BF16) if n == 0 else part
    spend(0.9)
    for pair in range(2):
        q2, k2, v2 = (lanes(qkv, pair, n) for n in range(3))
        for h in range(2):
            scores = nt(own(q2, h), k2) + S["bias"][...]
            row_max = jnp.max(scores, axis=1, keepdims=True)
            expon = jnp.exp(scores - row_max)
            probs = expon * (1.0 / jnp.sum(expon, axis=1, keepdims=True))
            S["probs"][slot, 2 * pair + h] = probs
            S["low"][h] = probs.astype(BF16)
        att = sum(nn(S["low"][h], own(v2, h)) for h in range(2))
        S["att"][g, :, pair * 128 : pair * 128 + 128] = att.astype(BF16)
        spend(1.0)


def backward(S, g, spend):
    qkv, slot = S["qkv"].at[g % 2], g % 2
    for pair in range(2):
        q2, k2, v2 = (lanes(qkv, pair, n) for n in range(3))
        o2 = S["ga"][g, :, pair * 128 : pair * 128 + 128]
        for h in range(2):
            probs = S["probs"][slot, 2 * pair + h]
            grad_probs = nt(own(o2, h), v2)
            delta = jnp.sum(probs * grad_probs, axis=1, keepdims=True)
            S["dscores"][h] = (probs * (grad_probs - delta)).astype(BF16)
            S["low"][h] = probs.astype(BF16)
        spend(0.8)
        dv = sum(tn(S["low"][h], own(o2, h)) for h in range(2))
        dq = sum(nn(S["dscores"][h], own(k2, h)) for h in range(2)) * 0.125
        dk = sum(tn(S["dscores"][h], own(q2, h)) for h in range(2))
        for n, part in enumerate((dq, dk, dv)):
            start = n * 256 + pair * 128
            S["dqkv"][:, start : start + 128] = part.astype(BF16)
        spend(0.8)


def weight_grads(S, g, spend):
    for m in range(4):
        if m:
            spend(0.25)
        part = nn(S["hidden_t"][m * 256 : m * 256 + 256], S["dqkv"][...]).astype(BF16)
        part = part.reshape(4, 2, 2, 16, 768)
        for r in range(2):
            for k in range(2):
                S["G"][g, m, :, :, 2 * r + k] = part[:, :, r, :, k * 384 : k * 384 + 384]


def hidden_grads(S, g, spend):
    for n in range(4):
        part = nt(S["dqkv"][...], S[f"W{g}"][n, :, :, :, 0:768].reshape(256, 768))
        columns = slice(n * 256, n * 256 + 256)
        S["gh"][:, columns] = part if g == 0 else S["gh"][:, columns] + part
        spend(0.2)


def proj_grads(S):
    for g in range(4):
        part = tn(S["att"][g], S["mcot"][...]).astype(BF16).reshape(4, 2, 2, 16, 1024)
        for r in range(2):
            for k in range(2):
                S["Gp"][g, :, :, 2 * r + k] = part[:, :, r, :, k * 512 : k * 512 + 512]


def small_grads(S):
    gh = S["gh"][...]
    gain_term = jnp.sum(gh * S["normed"][...], axis=0, keepdims=True)
    shift_term = jnp.sum(gh, axis=0, keepdims=True)
    for r in range(8):
        S["sums"][r : r + 1, :] = gain_term[:, r * 128 : r * 128 + 128]
        S["sums"][8 + r : 9 + r, :] = shift_term[:, r * 128 : r * 128 + 128]
    S["tile"][0] = S["sums"][...].astype(BF16)


def token_grads(S):
    normed = S["normed"][...]
    grad_normed = S["gh"][...] * S["gains"][0:1, :]
    inner = grad_normed - jnp.mean(grad_normed, axis=1, keepdims=True)
    inner = inner - normed * jnp.mean(grad_normed * normed, axis=1, keepdims=True)
    S["tokens"][...] = (S["cot"][...].astype(F32) + S["inverse"][:, 0:1] * inner).astype(BF16)


COMM = {}
for _name, _shape in reduce_shapes(384).items():
    COMM["g_" + _name] = ((4,) + _shape, BF16)
for _name, _shape in reduce_shapes(512).items():
    COMM["p_" + _name] = (_shape, BF16)
for _g, _width in enumerate((896, 768, 768, 768)):
    COMM[f"W{_g}"] = ((4, 4, 2, 32, _width), BF16)
COMM["Wp"] = ((4, 4, 2, 32, 1024), BF16)
COMM["G"] = ((4, 4, 4, 2, 4, 16, 384), BF16)
COMM["Gp"] = ((4, 4, 2, 4, 16, 512), BF16)
COMM["tile"] = ((4, 16, 128), BF16)
COMM["slots"] = ((4, 8, 16, 128), BF16)


def kernel(
    count_ref,
    starts_ref,
    tok_ref,
    cot_ref,
    qkv_ref,
    proj_ref,
    gain_ref,
    shift_ref,
    out_ref,
    qkv_out,
    proj_out,
    gain_out,
    shift_out,
    *scratch,
):
    S = dict(zip(tuple(SCRATCH) + tuple(COMM), scratch))
    gs, gr, rs, rr, ss, sr, ls = scratch[len(S) :]
    place = Place()
    x, z, c = place.x, place.zlo, place.c
    time = Timeline()

    def prepare():
        into = [(tok_ref, S["tokens"]), (cot_ref, S["cot"]), (proj_ref, S["Wp"].at[x, z, c])]
        into = [pltpu.make_async_copy(a, b, ls.at[n]) for n, (a, b) in enumerate(into)]
        for copy in into:
            copy.start()
        for g in range(4):
            for part in range(3):
                pltpu.make_async_copy(
                    qkv_ref.at[:, pl.ds(part * 1024 + g * 256, 256)],
                    S[f"W{g}"].at[x, z, c, :, pl.ds(part * 256, 256)],
                    ls.at[3 + g],
                ).start()
        own_small(S, gain_ref, shift_ref)
        last = S["W0"].at[x, z, c, :, pl.ds(768, 128)]
        last = pltpu.make_async_copy(S["own_low"], last, ls.at[7])
        last.start()
        into[0].wait()
        into[1].wait()
        prologue_tokens(S, count_ref, starts_ref)
        into[2].wait()
        last.wait()
        for g in range(4):
            own = S[f"W{g}"].at[x, z, c, :, pl.ds(0, 768)]
            pltpu.make_async_copy(own, own, ls.at[3 + g]).wait()

    enter(place.all(), prepare)

    buffers = [S[f"W{g}"] for g in range(4)] + [S["Wp"]]
    gathers = [Gather(place, b, k in DIRECT, gs.at[k], gr.at[k]) for k, b in enumerate(buffers)]

    def gather(k, start):
        piece = gathers[k]
        calls = (piece.stage0, piece.stage1, piece.stage2, piece.stage3, piece.stage4, piece.stage5)
        return time.add(zip(calls, DIRECT_TIMES if piece.direct else GATHER_TIMES), start)

    def write_group(g):
        def write(r, k, value):
            rows = slice(r * 16, r * 16 + 16)
            if k == 0:
                qkv_out[rows, g * 256 : g * 256 + 256] = value[:, 0:256]
                qkv_out[rows, 1024 + g * 256 : 1152 + g * 256] = value[:, 256:384]
            else:
                qkv_out[rows, 1152 + g * 256 : 1280 + g * 256] = value[:, 0:128]
                qkv_out[rows, 2048 + g * 256 : 2304 + g * 256] = value[:, 128:384]

        return write

    def write_proj(r, k, value):
        proj_out[r * 16 : r * 16 + 16, k * 512 : k * 512 + 512] = value

    def write_small(total):
        S["sums"][...] = total
        place_in_row = place.zlo * 2 + place.c
        for first, out in ((0, gain_out), (8, shift_out)):
            row = S["sums"][pl.ds(first + place.x * 2 + place.zlo // 2, 1), :]
            value = jnp.zeros((1, 32), F32)
            for k in range(4):
                value = jnp.where(place_in_row % 4 == k, row[:, k * 32 : k * 32 + 32], value)
            out[...] = value

    reduces = []

    def reduce(term, names, sem, write):
        piece = Reduce(place, term, names, rs.at[sem], rr.at[sem])
        reduces.append(piece)
        calls = (piece.stage0, piece.stage1, piece.stage2, piece.stage3, piece.stage4)
        calls += (piece.stage5, functools.partial(piece.stage6, write))
        return time.add(zip(calls, REDUCE_TIMES), 0.0, 1.5 if sem == 3 else 0.0)

    works = dict((k, gather(k, start)) for k, start in GATHER_STARTS)
    time.finish(works[0])
    prologue_hidden(S)
    time.spend(0.5)
    forward(S, 0, time.spend)
    time.finish(works[4])
    grads_attended(S)
    time.spend(1.0)
    for g in range(4):
        if 0 < g < 3:
            time.finish(works[g + 1])
            forward(S, g + 1, time.spend)
        if g == 2:
            proj_grads(S)
            reduce(S["Gp"], [S["p_" + n] for n in REDUCE_NAMES], 4, write_proj)
            time.spend(1.3)
        backward(S, g, time.spend)
        weight_grads(S, g, time.spend)
        names = [S["g_" + n].at[g] for n in REDUCE_NAMES]
        reduce(S["G"].at[g], names, g, write_group(g))
        hidden_grads(S, g, time.spend)
        if g == 0:
            time.finish(works[1])
            forward(S, 1, time.spend)
    small_grads(S)
    small = Small(place, S["tile"], S["slots"], ss, sr)
    calls = (small.stage0, small.stage1, small.stage2, small.stage3)
    calls += (functools.partial(small.stage4, write_small),)
    time.add(zip(calls, SMALL_TIMES))
    time.spend(0.3)
    token_grads(S)
    out = pltpu.make_async_copy(S["tokens"], out_ref, ls.at[0])
    out.start()
    time.spend(0.8)
    for work in list(time.live):
        time.finish(work)
    out.wait()
    for piece in gathers + reduces + [small]:
        piece.drain()


GATHER_STARTS = ((0, 0.0), (4, 3.4), (1, 8.0), (2, 11.5), (3, 15.0))
DIRECT = (0, 4)
DIRECT_TIMES = (3.4, 0.8, 6.0, 0.9, 2.0, 0.0)
GATHER_TIMES = (3.6, 0.8, 4.5, 4.0, 2.0, 0.0)
REDUCE_TIMES = (2.5, 4.5, 5.0, 4.5, 4.8, 30.0, 0.0)
SMALL_TIMES = (4.3, 5.3, 5.3, 30.0, 0.0)


LAST_SHAPES = (
    (ROWS, D, BF16, BF16),
    (32, 3072, BF16, F32),
    (32, 1024, BF16, F32),
    (1, 32, F32, F32),
    (1, 32, F32, F32),
)


def last_kernel(scale, *refs):
    ins, outs, scratch, sems = refs[:5], refs[5:10], refs[10:-1], refs[-1]
    before = scratch[:5]
    after = (scratch[0],) + scratch[5:]
    into = [pltpu.make_async_copy(a, b, sems.at[n]) for n, (a, b) in enumerate(zip(ins, before))]
    out = [pltpu.make_async_copy(a, b, sems.at[5 + n]) for n, (a, b) in enumerate(zip(after, outs))]
    for copy in into:
        copy.start()
    for n in (1, 2, 3, 4, 0):
        into[n].wait()
        if n:
            after[n][...] = before[n][...].astype(F32) * scale
        out[n].start()
    for copy in out:
        copy.wait()


def last(scale, *arrays):
    anyspace = pl.BlockSpec(memory_space=pl.ANY)
    return pl.pallas_call(
        functools.partial(last_kernel, scale),
        out_shape=[jax.ShapeDtypeStruct((r, c), t) for r, c, _, t in LAST_SHAPES],
        in_specs=[anyspace] * 5,
        out_specs=[anyspace] * 5,
        scratch_shapes=[pltpu.VMEM((r, c), t) for r, c, t, _ in LAST_SHAPES]
        + [pltpu.VMEM((r, c), t) for r, c, _, t in LAST_SHAPES[1:]]
        + [pltpu.SemaphoreType.DMA((10,))],
        name="last",
    )(*arrays)


def fused(counts, starts, tokens, cotangent, qkv_weight, proj_weight, gain, shift):
    anyspace = pl.BlockSpec(memory_space=pl.ANY)
    vmem = pl.BlockSpec(memory_space=pltpu.VMEM)
    smem = pl.BlockSpec(memory_space=pltpu.SMEM)
    buffers = tuple(SCRATCH.values()) + tuple(COMM.values())
    return pl.pallas_call(
        kernel,
        out_shape=[
            jax.ShapeDtypeStruct((ROWS, D), BF16),
            jax.ShapeDtypeStruct((32, 3072), BF16),
            jax.ShapeDtypeStruct((32, 1024), BF16),
            jax.ShapeDtypeStruct((1, 32), F32),
            jax.ShapeDtypeStruct((1, 32), F32),
        ],
        in_specs=[smem, smem] + [anyspace] * 4 + [vmem] * 2,
        out_specs=[anyspace] + [vmem] * 4,
        scratch_shapes=[pltpu.VMEM(*b) for b in buffers]
        + [
            pltpu.SemaphoreType.DMA((5, GATHER_SEMS[0])),
            pltpu.SemaphoreType.DMA((5, GATHER_SEMS[1])),
            pltpu.SemaphoreType.DMA((5, REDUCE_SEMS[0])),
            pltpu.SemaphoreType.DMA((5, REDUCE_SEMS[1])),
            pltpu.SemaphoreType.DMA((SMALL_SEMS[0],)),
            pltpu.SemaphoreType.DMA((SMALL_SEMS[1],)),
            pltpu.SemaphoreType.DMA((8,)),
        ],
        compiler_params=pltpu.CompilerParams(
            collective_id=0, has_side_effects=True, vmem_limit_bytes=67043328
        ),
        name="fused",
    )(counts, starts, tokens, cotangent, qkv_weight, proj_weight, gain, shift)


def per_device(
    tokens, cotangent, patch_count, image_starts, qkv_weight, proj_weight, norm_gain, norm_shift
):
    everyone = lax.axis_size("dp") * lax.axis_size("fsdp")
    scale = 1.0 / math.sqrt(tokens.shape[0] * everyone)
    sums = fused(
        patch_count,
        image_starts,
        tokens,
        cotangent,
        qkv_weight,
        proj_weight,
        norm_gain.reshape(1, -1),
        norm_shift.reshape(1, -1),
    )
    grad_block, qkv_grad, proj_grad, gain_grad, shift_grad = last(scale, *sums)
    return (grad_block, qkv_grad, proj_grad, gain_grad.reshape(-1), shift_grad.reshape(-1))


def solution(mesh):
    placed = (
        P(("dp", "fsdp"), None),
        P(("dp", "fsdp"), None),
        P(("dp", "fsdp")),
        P(("dp", "fsdp"), None),
        P("fsdp", None),
        P("fsdp", None),
        P("fsdp"),
        P("fsdp"),
    )
    return jax.shard_map(
        per_device,
        mesh=mesh,
        in_specs=placed,
        out_specs=(P(("dp", "fsdp"), None), P("fsdp", None), P("fsdp", None), P("fsdp"), P("fsdp")),
        check_vma=False,
    )
```

```python
import functools
import math

import jax
import jax.numpy as jnp
from jax import lax
from jax.experimental import pallas as pl
from jax.experimental.pallas import tpu as pltpu
from jax.sharding import PartitionSpec as P

MESH = pl.DeviceIdType.MESH
F32 = jnp.float32
BF16 = jnp.bfloat16
D = 1024
ROWS = 384


def nn(a, b):
    return lax.dot_general(a, b, (((1,), (0,)), ((), ())), preferred_element_type=F32)


def nt(a, b):
    return lax.dot_general(a, b, (((1,), (1,)), ((), ())), preferred_element_type=F32)


def tn(a, b):
    return lax.dot_general(a, b, (((0,), (0,)), ((), ())), preferred_element_type=F32)


class Place:
    def __init__(self):
        dp, fsdp = lax.axis_index("dp"), lax.axis_index("fsdp")
        self.y, self.zhi = dp // 2, dp % 2
        self.c = fsdp % 2
        chip = fsdp // 2
        self.x, self.zlo = chip // 4, chip % 4
        self.z = self.zhi * 4 + self.zlo

    def at(self, dx=0, dy=0, dz=0, flip=0):
        x = (self.x + dx + 4) % 4
        y = (self.y + dy + 4) % 4
        z = (self.z + dz + 8) % 8
        c = self.c + flip * (1 - 2 * self.c)
        return {"dp": y * 2 + z // 4, "fsdp": (x * 4 + z % 4) * 2 + c}

    def along_x(self, d):
        return self.at(dx=(1 - self.c) * d, dz=self.c * d)

    def along_z(self, d):
        return self.at(dx=self.c * d, dz=(1 - self.c) * d)

    def chip(self, i, j):
        x = (self.x + (1 - self.c) * i + self.c * j + 8) % 4
        z = (self.zlo + self.c * i + (1 - self.c) * j + 8) % 4
        return x, z

    def sibling(self):
        return self.at(flip=1)

    def first(self, d):
        return self.at(dx=self.c * d, dy=(1 - self.c) * d)

    def second(self, d):
        return self.at(dx=(1 - self.c) * d, dy=self.c * d)

    def quarter(self, d1, d2):
        x = (self.x + self.c * d1 + (1 - self.c) * d2) % 4
        y = (self.y + (1 - self.c) * d1 + self.c * d2) % 4
        return x, y

    def all(self):
        return (
            [self.sibling()]
            + [self.at(dx=d) for d in (1, 2, 3)]
            + [self.at(dy=d) for d in (1, 2, 3)]
            + [self.at(dz=d) for d in range(1, 8)]
        )


def enter(devices, meanwhile):
    barrier = pltpu.get_barrier_semaphore()
    for device in devices:
        pl.semaphore_signal(barrier, inc=1, device_id=device, device_id_type=MESH)
    meanwhile()
    pl.semaphore_wait(barrier, len(devices))


class Copies:
    def __init__(self, place, send_sems, recv_sems):
        self.place, self.send_sems, self.recv_sems = place, send_sems, recv_sems

    def copy(self, src, dst, out, into, device):
        return pltpu.make_async_remote_copy(
            src_ref=src,
            dst_ref=dst,
            send_sem=self.send_sems.at[out],
            recv_sem=self.recv_sems.at[into],
            device_id=device,
            device_id_type=MESH,
        )

    def start(self, src, dst, out, into, device):
        self.copy(src, dst, out, into, device).start()

    def arrived(self, ref, into):
        self.copy(ref, ref, 0, into, self.place.sibling()).wait_recv()

    def left(self, ref, out):
        self.copy(ref, ref, out, 0, self.place.sibling()).wait_send()


GATHER_SEMS = (3, 13)
ORDER = (0, -1, 1, 2)


class Gather(Copies):
    def __init__(self, place, buffer, direct, send_sems, recv_sems):
        super().__init__(place, send_sems, recv_sems)
        self.buffer, self.direct = buffer, direct

    def block(self, i, j, half=None):
        x, z = self.place.chip(i, j)
        ref = self.buffer.at[x, z, self.place.c]
        return ref if half is None else ref.at[pl.ds(half * 16, 16)]

    def forward(self, ref, out, into, device):
        self.start(ref, ref, out, into, device)

    def to_second(self, i):
        k = 3 + 2 * (i % 4)
        self.forward(self.block(i, 0), 1, k, self.place.along_z(1))
        self.forward(self.block(i, 0), 1, k + 1, self.place.along_z(-1))
        if self.direct:
            self.forward(self.block(i, 0, 0), 1, 11, self.place.along_z(2))
            self.forward(self.block(i, 0, 1), 1, 11, self.place.along_z(-2))
        self.to_sibling(i, 0)

    def to_sibling(self, i, j):
        self.forward(self.block(i, j), 2, 12, self.place.sibling())

    def stage0(self):
        self.forward(self.block(0, 0), 0, 0, self.place.along_x(1))
        self.forward(self.block(0, 0), 0, 1, self.place.along_x(-1))
        self.forward(self.block(0, 0, 0), 0, 2, self.place.along_x(2))
        self.forward(self.block(0, 0, 1), 0, 2, self.place.along_x(-2))
        self.to_second(0)

    def stage1(self):
        self.arrived(self.block(-1, 0), 0)
        self.to_second(-1)
        self.arrived(self.block(1, 0), 1)
        self.to_second(1)

    def stage2(self):
        self.arrived(self.block(2, 0), 2)
        self.to_second(2)

    def stage3(self):
        for i in ORDER:
            k = 3 + 2 * (i % 4)
            self.arrived(self.block(i, -1), k)
            if not self.direct:
                self.forward(self.block(i, -1, 0), 1, 11, self.place.along_z(1))
            self.to_sibling(i, -1)
            self.arrived(self.block(i, 1), k + 1)
            if not self.direct:
                self.forward(self.block(i, 1, 1), 1, 11, self.place.along_z(-1))
            self.to_sibling(i, 1)

    def stage4(self):
        self.arrived(self.buffer.at[0, :, 0], 11)
        for i in ORDER:
            self.to_sibling(i, 2)

    def stage5(self):
        self.arrived(self.buffer.at[:, :, 1 - self.place.c], 12)

    def drain(self):
        self.left(self.buffer.at[0, pl.ds(0, 3), 0], 0)
        self.left(self.buffer.at[pl.ds(0, 3), :, 0], 1)
        self.left(self.buffer.at[:, :, 0], 2)


REDUCE_SEMS = (5, 8)


def reduce_shapes(half):
    return dict(
        R=(4, 4, 4, 16, half),
        A=(4, 4, 4, 16, half),
        T=(2, 2, 4, 16, half),
        U=(2, 4, 4, 16, half),
        B=(4, 4, 16, half),
        Y=(3, 4, 16, half),
        C=(4, 16, half),
        V=(8, 16, half),
        E=(16, half),
        O=(4, 16, half),
    )


REDUCE_NAMES = tuple(reduce_shapes(128))


class Reduce(Copies):
    def __init__(self, place, term, buffers, send_sems, recv_sems):
        super().__init__(place, send_sems, recv_sems)
        self.term = term
        for name, ref in zip(REDUCE_NAMES, buffers):
            setattr(self, name, ref)

    def stage0(self):
        at = self.place

        @pl.when(at.c == 1)
        def _():
            for d1 in (2, 1, 3, 0):
                src = self.term.at[:, :, 0, (at.y + d1) % 4]
                self.start(src, self.R.at[d1], 0, 0 if d1 == 2 else 1, at.sibling())

        @pl.when(at.c == 0)
        def _():
            for d1 in (2, 1, 3, 0):
                src = self.term.at[(at.x + d1) % 4, :, 1]
                self.start(src, self.R.at[d1], 0, 0 if d1 == 2 else 1, at.sibling())

    def pair(self, d1):
        at = self.place
        for d2 in range(4):
            x, y = at.quarter(d1, d2)
            for z in range(4):
                m = (1 - at.c) * x + at.c * z
                n = (1 - at.c) * z + at.c * y
                both = self.term[x, z, at.c, y].astype(F32) + self.R[d1, m, n].astype(F32)
                self.A[d1, d2, z] = both.astype(BF16)

    def stage1(self):
        at = self.place
        self.arrived(self.R.at[2], 0)
        self.pair(2)
        self.start(self.A.at[2, pl.ds(0, 2)], self.T.at[0], 1, 2, at.first(1))
        self.start(self.A.at[2, pl.ds(2, 2)], self.T.at[1], 1, 3, at.first(-1))
        self.arrived(self.R.at[pl.ds(0, 3)], 1)
        self.pair(1)
        self.give(0, 1, 2, at.first(1))
        self.pair(3)
        self.give(1, 3, 0, at.first(-1))
        self.pair(0)

    def give(self, slot, d1, d2, device):
        half = pl.ds(d2, 2)
        self.start(self.A.at[d1, half], self.U.at[slot, half], 1, 4, device)

    def stage2(self):
        at = self.place
        self.arrived(self.T.at[0], 2)
        self.A[1, 0:2] = (self.A[1, 0:2].astype(F32) + self.T[0].astype(F32)).astype(BF16)
        self.give(0, 1, 0, at.first(1))
        self.arrived(self.T.at[1], 3)
        self.A[3, 2:4] = (self.A[3, 2:4].astype(F32) + self.T[1].astype(F32)).astype(BF16)
        self.give(1, 3, 2, at.first(-1))

    def stage3(self):
        at = self.place
        self.arrived(self.U, 4)
        for d2 in (2, 1, 3, 0):
            total = self.A[0, d2].astype(F32) + self.U[0, d2].astype(F32)
            self.B[d2] = (total + self.U[1, d2].astype(F32)).astype(BF16)
            if d2:
                self.start(self.B.at[d2], self.Y.at[d2 - 1], 2, 5, at.second(d2))

    def stage4(self):
        at = self.place
        self.arrived(self.Y, 5)
        total = self.B[0].astype(F32) + self.Y[0].astype(F32)
        total = total + self.Y[1].astype(F32) + self.Y[2].astype(F32)
        self.C[...] = total.astype(BF16)
        for d in (4, 3, 5, 2, 6, 1, 7):
            self.start(self.C.at[(at.zlo + d) % 4], self.V.at[at.z], 3, 6, at.at(dz=d))
        self.V[at.z] = self.C[at.zlo]

    def stage5(self):
        at = self.place
        self.arrived(self.V.at[pl.ds(0, 7)], 6)
        total = self.V[0].astype(F32)
        for z in range(1, 8):
            total = total + self.V[z].astype(F32)
        self.E[...] = total.astype(BF16)
        for d in (2, 1, 3):
            self.start(self.E, self.O.at[at.y], 4, 7, at.at(dy=d))

    def stage6(self, write):
        at = self.place
        self.arrived(self.O.at[pl.ds(0, 3)], 7)
        self.O[at.y] = self.E[...]
        for r in range(2):
            for k in range(2):
                write(r, k, self.O[2 * r + k])

    def drain(self):
        self.left(self.R, 0)
        self.left(self.A.at[pl.ds(0, 3)], 1)
        self.left(self.A.at[0, pl.ds(0, 3)], 2)
        self.left(self.V.at[pl.ds(0, 7)], 3)
        self.left(self.O.at[pl.ds(0, 3)], 4)


SMALL_SEMS = (4, 4)


class Small(Copies):
    def __init__(self, place, tile, slots, send_sems, recv_sems):
        super().__init__(place, send_sems, recv_sems)
        self.tile, self.slots = tile, slots

    def step(self, n):
        at = self.place
        size, mine = ((4, at.x), (4, at.y), (8, at.z), (2, at.c))[n]
        other = (
            lambda d: at.at(dx=d),
            lambda d: at.at(dy=d),
            lambda d: at.at(dz=d),
            lambda d: at.sibling(),
        )[n]
        return size, mine, other

    def send(self, n):
        size, mine, other = self.step(n)
        for d in range(1, size):
            self.start(self.tile.at[n], self.slots.at[n, mine], n, n, other(d))

    def receive(self, n):
        size, mine, _ = self.step(n)
        self.arrived(self.slots.at[n, pl.ds(0, size - 1)], n)
        self.slots[n, mine] = self.tile[n]
        total = self.slots[n, 0].astype(F32)
        for k in range(1, size):
            total = total + self.slots[n, k].astype(F32)
        return total

    def stage0(self):
        self.send(0)

    def stage1(self):
        self.tile[1] = self.receive(0).astype(BF16)
        self.send(1)

    def stage2(self):
        self.tile[2] = self.receive(1).astype(BF16)
        self.send(2)

    def stage3(self):
        self.tile[3] = self.receive(2).astype(BF16)
        self.send(3)

    def stage4(self, write):
        write(self.receive(3))

    def drain(self):
        for n in range(4):
            self.left(self.slots.at[n, pl.ds(0, self.step(n)[0] - 1)], n)


class Timeline:
    def __init__(self):
        self.now, self.live = 0.0, []

    def add(self, stages, start=0.0, first=0.0):
        work = [max(start, self.now), first, len(self.live), list(stages)]
        self.live.append(work)
        self.run(self.now)
        return work

    def step(self, work):
        call, latency = work[3].pop(0)
        call()
        work[0] = max(self.now, work[0]) + latency

    def run(self, until):
        while True:
            ready = [w for w in self.live if w[3] and w[0] <= until]
            if not ready:
                return
            self.step(min(ready, key=lambda w: (w[0] - w[1], w[2])))

    def spend(self, time):
        self.now += time
        self.run(self.now)

    def finish(self, work):
        while work[3]:
            self.now = max(self.now, min(w[0] for w in self.live if w[3]))
            self.run(self.now)


SCRATCH = {
    "normed": ((384, 1024), F32),
    "inverse": ((384, 128), F32),
    "hidden": ((384, 1024), BF16),
    "hidden_t": ((1024, 384), BF16),
    "mcot": ((384, 1024), BF16),
    "live": ((384, 128), F32),
    "ga": ((4, 384, 256), BF16),
    "att": ((4, 384, 256), BF16),
    "qkv": ((2, 384, 768), BF16),
    "dqkv": ((4, 384, 768), BF16),
    "bias": ((384, 384), F32),
    "gains": ((2, 1024), F32),
    "probs": ((2, 4, 384, 384), F32),
    "low": ((2, 384, 384), BF16),
    "dscores": ((2, 384, 384), BF16),
    "gh": ((384, 1024), F32),
    "tokens": ((384, 1024), BF16),
    "cot": ((384, 1024), BF16),
    "own": ((128, 128), F32),
    "own_low": ((32, 128), BF16),
    "sums": ((16, 128), F32),
    "gain": ((1, 32), BF16),
    "shift": ((1, 32), BF16),
}


def own_small(S):
    S["own"][...] = jnp.zeros((128, 128), F32)
    S["own"][0:1, 0:32] = S["gain"][...].astype(F32)
    S["own"][1:2, 0:32] = S["shift"][...].astype(F32)
    S["own_low"][...] = S["own"][...].T[0:32].astype(BF16)


def prologue_tokens(S, count_ref, starts_ref):
    source = S["tokens"][...].astype(F32)
    center = jnp.mean(source, axis=1, keepdims=True)
    centered = source - center
    variance = jnp.mean(centered * centered, axis=1, keepdims=True)
    inverse = lax.rsqrt(variance + 1e-06)
    S["normed"][...] = centered * inverse
    S["inverse"][...] = jnp.broadcast_to(inverse, (ROWS, 128))
    count = count_ref[0]
    down = lax.broadcasted_iota(jnp.int32, (ROWS, 1), 0)
    across = lax.broadcasted_iota(jnp.int32, (1, ROWS), 1)
    seg_down = jnp.zeros((ROWS, 1), jnp.int32)
    seg_across = jnp.zeros((1, ROWS), jnp.int32)
    for j in range(8):
        start = starts_ref[0, j]
        seg_down = seg_down + jnp.where(down >= start, 1, 0)
        seg_across = seg_across + jnp.where(across >= start, 1, 0)
    seg_down = jnp.where(down < count, seg_down, -1)
    seg_across = jnp.where(across < count, seg_across, -2)
    S["bias"][...] = jnp.where(seg_down == seg_across, 0.0, -1e30).astype(F32)
    alive = lax.broadcasted_iota(jnp.int32, (ROWS, 128), 0) < count
    S["live"][...] = jnp.where(alive, 1.0, 0.0).astype(F32)
    alive = S["live"][:, 0:1] > 0.5
    S["mcot"][...] = jnp.where(alive, S["cot"][...].astype(F32), 0.0).astype(BF16)


def prologue_hidden(S):
    small = S["W0"][:, :, :, :, 768:896].reshape(1024, 128).astype(F32)
    S["gains"][...] = small.T[0:2, :]
    gain = S["gains"][0:1, :]
    shift = S["gains"][1:2, :]
    S["hidden"][...] = (S["normed"][...] * gain + shift).astype(BF16)
    S["hidden_t"][...] = S["hidden"][...].T


def grads_attended(S):
    for g in range(4):
        part = S["Wp"][g].reshape(256, 1024)
        S["ga"][g] = nt(S["mcot"][...], part).astype(BF16)


def own(a, h):
    first = lax.broadcasted_iota(jnp.int32, (ROWS, 128), 1) < 64
    zero = jnp.zeros_like(a)
    return jnp.where(first, a, zero) if h == 0 else jnp.where(first, zero, a)


def lanes(ref, pair, part):
    return ref[:, part * 256 + pair * 128 : part * 256 + pair * 128 + 128]


def forward(S, g, spend):
    qkv, slot = S["qkv"].at[g % 2], g % 2
    for n in range(3):
        weight = S[f"W{g}"][:, :, :, :, n * 256 : n * 256 + 256].reshape(1024, 256)
        part = nn(S["hidden"][...], weight).astype(BF16)
        qkv[:, n * 256 : n * 256 + 256] = part * jnp.asarray(0.125, BF16) if n == 0 else part
    spend(0.8)
    for pair in range(2):
        q2, k2, v2 = (lanes(qkv, pair, n) for n in range(3))
        for h in range(2):
            scores = nt(own(q2, h), k2) + S["bias"][...]
            row_max = jnp.max(scores, axis=1, keepdims=True)
            expon = jnp.exp(scores - row_max)
            probs = expon * (1.0 / jnp.sum(expon, axis=1, keepdims=True))
            S["probs"][slot, 2 * pair + h] = probs
            S["low"][h] = probs.astype(BF16)
        att = sum(nn(S["low"][h], own(v2, h)) for h in range(2))
        S["att"][g, :, pair * 128 : pair * 128 + 128] = att.astype(BF16)
        spend(0.85)


def backward(S, g, spend):
    qkv, slot = S["qkv"].at[g % 2], g % 2
    for pair in range(2):
        q2, k2, v2 = (lanes(qkv, pair, n) for n in range(3))
        o2 = S["ga"][g, :, pair * 128 : pair * 128 + 128]
        for h in range(2):
            probs = S["probs"][slot, 2 * pair + h]
            grad_probs = nt(own(o2, h), v2)
            delta = jnp.sum(probs * grad_probs, axis=1, keepdims=True)
            S["dscores"][h] = (probs * (grad_probs - delta)).astype(BF16)
            S["low"][h] = probs.astype(BF16)
        spend(0.55)
        dv = sum(tn(S["low"][h], own(o2, h)) for h in range(2))
        dq = sum(nn(S["dscores"][h], own(k2, h)) for h in range(2)) * 0.125
        dk = sum(tn(S["dscores"][h], own(q2, h)) for h in range(2))
        for n, part in enumerate((dq, dk, dv)):
            start = n * 256 + pair * 128
            S["dqkv"][g, :, start : start + 128] = part.astype(BF16)
        spend(0.55)


def weight_grads(S, g, spend):
    for m in range(4):
        if m:
            spend(0.25)
        part = nn(S["hidden_t"][m * 256 : m * 256 + 256], S["dqkv"][g]).astype(BF16)
        part = part.reshape(4, 2, 2, 16, 768)
        for r in range(2):
            for k in range(2):
                S["G"][g, m, :, :, 2 * r + k] = part[:, :, r, :, k * 384 : k * 384 + 384]


def hidden_grads(S, spend):
    for n in range(4):
        S["gh"][:, n * 256 : n * 256 + 256] = sum(
            nt(S["dqkv"][g], S[f"W{g}"][n, :, :, :, 0:768].reshape(256, 768)) for g in range(4)
        )
        spend(1.15)


def proj_grads(S):
    for g in range(4):
        part = tn(S["att"][g], S["mcot"][...]).astype(BF16).reshape(4, 2, 2, 16, 1024)
        for r in range(2):
            for k in range(2):
                S["Gp"][g, :, :, 2 * r + k] = part[:, :, r, :, k * 512 : k * 512 + 512]


def small_grads(S):
    gh = S["gh"][...]
    gain_term = jnp.sum(gh * S["normed"][...], axis=0, keepdims=True)
    shift_term = jnp.sum(gh, axis=0, keepdims=True)
    for r in range(8):
        S["sums"][r : r + 1, :] = gain_term[:, r * 128 : r * 128 + 128]
        S["sums"][8 + r : 9 + r, :] = shift_term[:, r * 128 : r * 128 + 128]
    S["tile"][0] = S["sums"][...].astype(BF16)


def token_grads(S):
    normed = S["normed"][...]
    grad_normed = S["gh"][...] * S["gains"][0:1, :]
    inner = grad_normed - jnp.mean(grad_normed, axis=1, keepdims=True)
    inner = inner - normed * jnp.mean(grad_normed * normed, axis=1, keepdims=True)
    S["tokens"][...] = (S["cot"][...].astype(F32) + S["inverse"][:, 0:1] * inner).astype(BF16)


COMM = {}
for _name, _shape in reduce_shapes(384).items():
    COMM["g_" + _name] = ((4,) + _shape, BF16)
for _name, _shape in reduce_shapes(512).items():
    COMM["p_" + _name] = (_shape, BF16)
for _g, _width in enumerate((896, 768, 768, 768)):
    COMM[f"W{_g}"] = ((4, 4, 2, 32, _width), BF16)
COMM["Wp"] = ((4, 4, 2, 32, 1024), BF16)
COMM["G"] = ((4, 4, 4, 2, 4, 16, 384), BF16)
COMM["Gp"] = ((4, 4, 2, 4, 16, 512), BF16)
COMM["tile"] = ((4, 16, 128), BF16)
COMM["slots"] = ((4, 8, 16, 128), BF16)


def kernel(
    count_ref,
    starts_ref,
    tok_ref,
    cot_ref,
    qkv_ref,
    proj_ref,
    gain_ref,
    shift_ref,
    out_ref,
    qkv_out,
    proj_out,
    gain_out,
    shift_out,
    *scratch,
):
    S = dict(zip(tuple(SCRATCH) + tuple(COMM), scratch))
    gs, gr, rs, rr, ss, sr, ls, count, starts = scratch[len(S) :]
    place = Place()
    x, z, c = place.x, place.zlo, place.c
    time = Timeline()

    def prepare():
        few = (count_ref, count), (starts_ref, starts), (gain_ref, S["gain"]), (shift_ref, S["shift"])
        few = [pltpu.make_async_copy(a, b, ls.at[8 + n]) for n, (a, b) in enumerate(few)]
        for copy in few:
            copy.start()
        into = [(tok_ref, S["tokens"]), (cot_ref, S["cot"]), (proj_ref, S["Wp"].at[x, z, c])]
        into = [pltpu.make_async_copy(a, b, ls.at[n]) for n, (a, b) in enumerate(into)]
        for copy in into:
            copy.start()
        for g in range(4):
            for part in range(3):
                pltpu.make_async_copy(
                    qkv_ref.at[:, pl.ds(part * 1024 + g * 256, 256)],
                    S[f"W{g}"].at[x, z, c, :, pl.ds(part * 256, 256)],
                    ls.at[3 + g],
                ).start()
        for copy in few:
            copy.wait()
        own_small(S)
        last = S["W0"].at[x, z, c, :, pl.ds(768, 128)]
        last = pltpu.make_async_copy(S["own_low"], last, ls.at[7])
        last.start()
        into[0].wait()
        into[1].wait()
        prologue_tokens(S, count, starts)
        into[2].wait()
        last.wait()
        for g in range(4):
            own = S[f"W{g}"].at[x, z, c, :, pl.ds(0, 768)]
            pltpu.make_async_copy(own, own, ls.at[3 + g]).wait()

    enter(place.all(), prepare)

    buffers = [S[f"W{g}"] for g in range(4)] + [S["Wp"]]
    gathers = [Gather(place, b, k in DIRECT, gs.at[k], gr.at[k]) for k, b in enumerate(buffers)]

    def gather(k, start):
        piece = gathers[k]
        calls = (piece.stage0, piece.stage1, piece.stage2, piece.stage3, piece.stage4, piece.stage5)
        return time.add(zip(calls, DIRECT_TIMES if piece.direct else GATHER_TIMES), start)

    def write_group(g):
        def write(r, k, value):
            rows = slice(r * 16, r * 16 + 16)
            if k == 0:
                qkv_out[rows, g * 256 : g * 256 + 256] = value[:, 0:256]
                qkv_out[rows, 1024 + g * 256 : 1152 + g * 256] = value[:, 256:384]
            else:
                qkv_out[rows, 1152 + g * 256 : 1280 + g * 256] = value[:, 0:128]
                qkv_out[rows, 2048 + g * 256 : 2304 + g * 256] = value[:, 128:384]

        return write

    def write_proj(r, k, value):
        proj_out[r * 16 : r * 16 + 16, k * 512 : k * 512 + 512] = value

    def write_small(total):
        S["sums"][...] = total
        place_in_row = place.zlo * 2 + place.c
        for first, out in ((0, gain_out), (8, shift_out)):
            row = S["sums"][pl.ds(first + place.x * 2 + place.zlo // 2, 1), :]
            value = jnp.zeros((1, 32), F32)
            for k in range(4):
                value = jnp.where(place_in_row % 4 == k, row[:, k * 32 : k * 32 + 32], value)
            out[...] = value

    reduces = []

    def reduce(term, names, sem, write):
        piece = Reduce(place, term, names, rs.at[sem], rr.at[sem])
        reduces.append(piece)
        calls = (piece.stage0, piece.stage1, piece.stage2, piece.stage3, piece.stage4)
        calls += (piece.stage5, functools.partial(piece.stage6, write))
        final = sem == 3
        return time.add(zip(calls, REDUCE_TIMES[sem]), 0.0, 1.5 if final else 0.0)

    works = dict((k, gather(k, start)) for k, start in GATHER_STARTS)
    time.finish(works[0])
    prologue_hidden(S)
    time.spend(0.5)
    forward(S, 0, time.spend)
    time.finish(works[4])
    grads_attended(S)
    time.spend(1.0)
    for g in range(4):
        if 0 < g < 3:
            time.finish(works[g + 1])
            forward(S, g + 1, time.spend)
        if g == 2:
            proj_grads(S)
            reduce(S["Gp"], [S["p_" + n] for n in REDUCE_NAMES], 4, write_proj)
            time.spend(1.3)
        backward(S, g, time.spend)
        weight_grads(S, g, time.spend)
        names = [S["g_" + n].at[g] for n in REDUCE_NAMES]
        reduce(S["G"].at[g], names, g, write_group(g))
        time.spend(0.25)
        if g == 0:
            time.finish(works[1])
            forward(S, 1, time.spend)
    hidden_grads(S, time.spend)
    small_grads(S)
    small = Small(place, S["tile"], S["slots"], ss, sr)
    calls = (small.stage0, small.stage1, small.stage2, small.stage3)
    calls += (functools.partial(small.stage4, write_small),)
    time.add(zip(calls, SMALL_TIMES), 0.0, 1.0)
    time.spend(0.3)
    token_grads(S)
    out = pltpu.make_async_copy(S["tokens"], out_ref, ls.at[0])
    out.start()
    time.spend(0.8)
    for work in list(time.live):
        time.finish(work)
    out.wait()
    for piece in gathers + reduces + [small]:
        piece.drain()


GATHER_STARTS = ((0, 0.0), (4, 3.4), (1, 8.0), (2, 11.5), (3, 15.0))
DIRECT = (0, 4)
DIRECT_TIMES = (3.4, 0.8, 6.0, 0.9, 2.0, 0.0)
GATHER_TIMES = (3.6, 0.8, 4.5, 4.0, 2.0, 0.0)
EARLY = (2.5, 4.8, 5.0, 5.0, 5.5, 30.0, 0.0)
LATE = (2.0, 4.5, 5.5, 5.5, 5.0, 30.0, 0.0)
FINAL = (1.5, 4.3, 4.8, 4.2, 4.6, 30.0, 0.0)
REDUCE_TIMES = (EARLY, EARLY, LATE, FINAL, (4.3,) + LATE[1:])
SMALL_TIMES = (4.4, 4.6, 5.6, 25.0, 0.0)


LAST_SHAPES = (
    (ROWS, D, BF16, BF16),
    (32, 3072, BF16, F32),
    (32, 1024, BF16, F32),
    (1, 32, F32, F32),
    (1, 32, F32, F32),
)


def last_kernel(scale, *refs):
    ins, outs, scratch, sems = refs[:5], refs[5:10], refs[10:-1], refs[-1]
    before = scratch[:5]
    after = (scratch[0],) + scratch[5:]
    into = [pltpu.make_async_copy(a, b, sems.at[n]) for n, (a, b) in enumerate(zip(ins, before))]
    out = [pltpu.make_async_copy(a, b, sems.at[5 + n]) for n, (a, b) in enumerate(zip(after, outs))]
    for copy in into:
        copy.start()
    for n in (1, 2, 3, 4, 0):
        into[n].wait()
        if n:
            after[n][...] = before[n][...].astype(F32) * scale
        out[n].start()
    for copy in out:
        copy.wait()


def last(scale, *arrays):
    anyspace = pl.BlockSpec(memory_space=pl.ANY)
    return pl.pallas_call(
        functools.partial(last_kernel, scale),
        out_shape=[jax.ShapeDtypeStruct((r, c), t) for r, c, _, t in LAST_SHAPES],
        in_specs=[anyspace] * 5,
        out_specs=[anyspace] * 5,
        scratch_shapes=[pltpu.VMEM((r, c), t) for r, c, t, _ in LAST_SHAPES]
        + [pltpu.VMEM((r, c), t) for r, c, _, t in LAST_SHAPES[1:]]
        + [pltpu.SemaphoreType.DMA((10,))],
        name="last",
    )(*arrays)


def fused(counts, starts, tokens, cotangent, qkv_weight, proj_weight, gain, shift):
    anyspace = pl.BlockSpec(memory_space=pl.ANY)
    vmem = pl.BlockSpec(memory_space=pltpu.VMEM)
    buffers = tuple(SCRATCH.values()) + tuple(COMM.values())
    return pl.pallas_call(
        kernel,
        out_shape=[
            jax.ShapeDtypeStruct((ROWS, D), BF16),
            jax.ShapeDtypeStruct((32, 3072), BF16),
            jax.ShapeDtypeStruct((32, 1024), BF16),
            jax.ShapeDtypeStruct((1, 32), F32),
            jax.ShapeDtypeStruct((1, 32), F32),
        ],
        in_specs=[anyspace] * 8,
        out_specs=[anyspace] + [vmem] * 4,
        scratch_shapes=[pltpu.VMEM(*b) for b in buffers]
        + [
            pltpu.SemaphoreType.DMA((5, GATHER_SEMS[0])),
            pltpu.SemaphoreType.DMA((5, GATHER_SEMS[1])),
            pltpu.SemaphoreType.DMA((5, REDUCE_SEMS[0])),
            pltpu.SemaphoreType.DMA((5, REDUCE_SEMS[1])),
            pltpu.SemaphoreType.DMA((SMALL_SEMS[0],)),
            pltpu.SemaphoreType.DMA((SMALL_SEMS[1],)),
            pltpu.SemaphoreType.DMA((12,)),
            pltpu.SMEM((1,), jnp.int32),
            pltpu.SMEM((1, 8), jnp.int32),
        ],
        compiler_params=pltpu.CompilerParams(
            collective_id=0, has_side_effects=True, vmem_limit_bytes=67043328
        ),
        name="fused",
    )(counts, starts, tokens, cotangent, qkv_weight, proj_weight, gain, shift)


def per_device(
    tokens, cotangent, patch_count, image_starts, qkv_weight, proj_weight, norm_gain, norm_shift
):
    everyone = lax.axis_size("dp") * lax.axis_size("fsdp")
    scale = 1.0 / math.sqrt(tokens.shape[0] * everyone)
    sums = fused(
        patch_count,
        image_starts,
        tokens,
        cotangent,
        qkv_weight,
        proj_weight,
        norm_gain.reshape(1, -1),
        norm_shift.reshape(1, -1),
    )
    grad_block, qkv_grad, proj_grad, gain_grad, shift_grad = last(scale, *sums)
    return (grad_block, qkv_grad, proj_grad, gain_grad.reshape(-1), shift_grad.reshape(-1))


def solution(mesh):
    placed = (
        P(("dp", "fsdp"), None),
        P(("dp", "fsdp"), None),
        P(("dp", "fsdp")),
        P(("dp", "fsdp"), None),
        P("fsdp", None),
        P("fsdp", None),
        P("fsdp"),
        P("fsdp"),
    )
    return jax.shard_map(
        per_device,
        mesh=mesh,
        in_specs=placed,
        out_specs=(P(("dp", "fsdp"), None), P("fsdp", None), P("fsdp", None), P("fsdp"), P("fsdp")),
        check_vma=False,
    )
```

```python
import functools
import math

import jax
import jax.numpy as jnp
from jax import lax
from jax.experimental import pallas as pl
from jax.experimental.pallas import tpu as pltpu
from jax.sharding import PartitionSpec as P

MESH = pl.DeviceIdType.MESH
F32 = jnp.float32
BF16 = jnp.bfloat16
D = 1024
ROWS = 384


def nn(a, b):
    return lax.dot_general(a, b, (((1,), (0,)), ((), ())), preferred_element_type=F32)


def nt(a, b):
    return lax.dot_general(a, b, (((1,), (1,)), ((), ())), preferred_element_type=F32)


def tn(a, b):
    return lax.dot_general(a, b, (((0,), (0,)), ((), ())), preferred_element_type=F32)


class Place:
    def __init__(self):
        dp, fsdp = lax.axis_index("dp"), lax.axis_index("fsdp")
        self.y, self.zhi = dp // 2, dp % 2
        self.c = fsdp % 2
        chip = fsdp // 2
        self.x, self.zlo = chip // 4, chip % 4
        self.z = self.zhi * 4 + self.zlo

    def at(self, dx=0, dy=0, dz=0, flip=0):
        x = (self.x + dx + 4) % 4
        y = (self.y + dy + 4) % 4
        z = (self.z + dz + 8) % 8
        c = self.c + flip * (1 - 2 * self.c)
        return {"dp": y * 2 + z // 4, "fsdp": (x * 4 + z % 4) * 2 + c}

    def along_x(self, d):
        return self.at(dx=(1 - self.c) * d, dz=self.c * d)

    def along_z(self, d):
        return self.at(dx=self.c * d, dz=(1 - self.c) * d)

    def chip(self, i, j):
        x = (self.x + (1 - self.c) * i + self.c * j + 8) % 4
        z = (self.zlo + self.c * i + (1 - self.c) * j + 8) % 4
        return x, z

    def sibling(self):
        return self.at(flip=1)

    def first(self, d):
        return self.at(dx=self.c * d, dy=(1 - self.c) * d)

    def second(self, d):
        return self.at(dx=(1 - self.c) * d, dy=self.c * d)

    def quarter(self, d1, d2):
        x = (self.x + self.c * d1 + (1 - self.c) * d2) % 4
        y = (self.y + (1 - self.c) * d1 + self.c * d2) % 4
        return x, y

    def all(self):
        return (
            [self.at(dz=d) for d in (4, 3, 5, 2, 6, 1, 7)]
            + [self.at(dy=d) for d in (2, 1, 3)]
            + [self.at(dx=d) for d in (2, 1, 3)]
            + [self.sibling()]
        )


def enter(devices, meanwhile):
    barrier = pltpu.get_barrier_semaphore()
    for device in devices:
        pl.semaphore_signal(barrier, inc=1, device_id=device, device_id_type=MESH)
    meanwhile()
    pl.semaphore_wait(barrier, len(devices))


class Copies:
    def __init__(self, place, send_sems, recv_sems):
        self.place, self.send_sems, self.recv_sems = place, send_sems, recv_sems

    def copy(self, src, dst, out, into, device):
        return pltpu.make_async_remote_copy(
            src_ref=src,
            dst_ref=dst,
            send_sem=self.send_sems.at[out],
            recv_sem=self.recv_sems.at[into],
            device_id=device,
            device_id_type=MESH,
        )

    def start(self, src, dst, out, into, device):
        self.copy(src, dst, out, into, device).start()

    def arrived(self, ref, into):
        self.copy(ref, ref, 0, into, self.place.sibling()).wait_recv()

    def left(self, ref, out):
        self.copy(ref, ref, out, 0, self.place.sibling()).wait_send()


GATHER_SEMS = (3, 13)
ORDER = (0, -1, 1, 2)


class Gather(Copies):
    def __init__(self, place, buffer, direct, send_sems, recv_sems):
        super().__init__(place, send_sems, recv_sems)
        self.buffer, self.direct = buffer, direct

    def block(self, i, j, half=None):
        x, z = self.place.chip(i, j)
        ref = self.buffer.at[x, z, self.place.c]
        return ref if half is None else ref.at[pl.ds(half * 16, 16)]

    def forward(self, ref, out, into, device):
        self.start(ref, ref, out, into, device)

    def to_second(self, i):
        k = 3 + 2 * (i % 4)
        self.forward(self.block(i, 0), 1, k, self.place.along_z(1))
        self.forward(self.block(i, 0), 1, k + 1, self.place.along_z(-1))
        if self.direct:
            self.forward(self.block(i, 0, 0), 1, 11, self.place.along_z(2))
            self.forward(self.block(i, 0, 1), 1, 11, self.place.along_z(-2))
        self.to_sibling(i, 0)

    def to_sibling(self, i, j):
        self.forward(self.block(i, j), 2, 12, self.place.sibling())

    def stage0(self):
        self.forward(self.block(0, 0), 0, 0, self.place.along_x(1))
        self.forward(self.block(0, 0), 0, 1, self.place.along_x(-1))
        self.forward(self.block(0, 0, 0), 0, 2, self.place.along_x(2))
        self.forward(self.block(0, 0, 1), 0, 2, self.place.along_x(-2))
        self.to_second(0)

    def stage1(self):
        self.arrived(self.block(-1, 0), 0)
        self.to_second(-1)
        self.arrived(self.block(1, 0), 1)
        self.to_second(1)

    def stage2(self):
        self.arrived(self.block(2, 0), 2)
        self.to_second(2)

    def stage3(self):
        for i in ORDER:
            k = 3 + 2 * (i % 4)
            self.arrived(self.block(i, -1), k)
            if not self.direct:
                self.forward(self.block(i, -1, 0), 1, 11, self.place.along_z(1))
            self.to_sibling(i, -1)
            self.arrived(self.block(i, 1), k + 1)
            if not self.direct:
                self.forward(self.block(i, 1, 1), 1, 11, self.place.along_z(-1))
            self.to_sibling(i, 1)

    def stage4(self):
        self.arrived(self.buffer.at[0, :, 0], 11)
        for i in ORDER:
            self.to_sibling(i, 2)

    def stage5(self):
        self.arrived(self.buffer.at[:, :, 1 - self.place.c], 12)

    def drain(self):
        self.left(self.buffer.at[0, pl.ds(0, 3), 0], 0)
        self.left(self.buffer.at[pl.ds(0, 3), :, 0], 1)
        self.left(self.buffer.at[:, :, 0], 2)


REDUCE_SEMS = (5, 8)


def reduce_shapes(half):
    return dict(
        R=(4, 4, 4, 16, half),
        A=(4, 4, 4, 16, half),
        T=(2, 2, 4, 16, half),
        U=(2, 4, 4, 16, half),
        B=(4, 4, 16, half),
        Y=(3, 4, 16, half),
        C=(4, 16, half),
        V=(8, 16, half),
        E=(16, half),
        O=(4, 16, half),
    )


REDUCE_NAMES = tuple(reduce_shapes(128))


class Reduce(Copies):
    def __init__(self, place, term, buffers, send_sems, recv_sems):
        super().__init__(place, send_sems, recv_sems)
        self.term = term
        for name, ref in zip(REDUCE_NAMES, buffers):
            setattr(self, name, ref)

    def stage0(self):
        at = self.place

        @pl.when(at.c == 1)
        def _():
            for d1 in (2, 1, 3, 0):
                src = self.term.at[:, :, 0, (at.y + d1) % 4]
                self.start(src, self.R.at[d1], 0, 0 if d1 == 2 else 1, at.sibling())

        @pl.when(at.c == 0)
        def _():
            for d1 in (2, 1, 3, 0):
                src = self.term.at[(at.x + d1) % 4, :, 1]
                self.start(src, self.R.at[d1], 0, 0 if d1 == 2 else 1, at.sibling())

    def pair(self, d1):
        at = self.place
        for d2 in range(4):
            x, y = at.quarter(d1, d2)
            for z in range(4):
                m = (1 - at.c) * x + at.c * z
                n = (1 - at.c) * z + at.c * y
                both = self.term[x, z, at.c, y].astype(F32) + self.R[d1, m, n].astype(F32)
                self.A[d1, d2, z] = both.astype(BF16)

    def stage1(self):
        at = self.place
        self.arrived(self.R.at[2], 0)
        self.pair(2)
        self.start(self.A.at[2, pl.ds(0, 2)], self.T.at[0], 1, 2, at.first(1))
        self.start(self.A.at[2, pl.ds(2, 2)], self.T.at[1], 1, 3, at.first(-1))
        self.arrived(self.R.at[pl.ds(0, 3)], 1)
        self.pair(1)
        self.give(0, 1, 2, at.first(1))
        self.pair(3)
        self.give(1, 3, 0, at.first(-1))
        self.pair(0)

    def give(self, slot, d1, d2, device):
        half = pl.ds(d2, 2)
        self.start(self.A.at[d1, half], self.U.at[slot, half], 1, 4, device)

    def stage2(self):
        at = self.place
        self.arrived(self.T.at[0], 2)
        self.A[1, 0:2] = (self.A[1, 0:2].astype(F32) + self.T[0].astype(F32)).astype(BF16)
        self.give(0, 1, 0, at.first(1))
        self.arrived(self.T.at[1], 3)
        self.A[3, 2:4] = (self.A[3, 2:4].astype(F32) + self.T[1].astype(F32)).astype(BF16)
        self.give(1, 3, 2, at.first(-1))

    def stage3(self):
        at = self.place
        self.arrived(self.U, 4)
        for d2 in (2, 1, 3, 0):
            total = self.A[0, d2].astype(F32) + self.U[0, d2].astype(F32)
            self.B[d2] = (total + self.U[1, d2].astype(F32)).astype(BF16)
            if d2:
                self.start(self.B.at[d2], self.Y.at[d2 - 1], 2, 5, at.second(d2))

    def stage4(self):
        at = self.place
        self.arrived(self.Y, 5)
        total = self.B[0].astype(F32) + self.Y[0].astype(F32)
        total = total + self.Y[1].astype(F32) + self.Y[2].astype(F32)
        self.C[...] = total.astype(BF16)
        for d in (4, 3, 5, 2, 6, 1, 7):
            self.start(self.C.at[(at.zlo + d) % 4], self.V.at[at.z], 3, 6, at.at(dz=d))
        self.V[at.z] = self.C[at.zlo]

    def stage5(self):
        at = self.place
        self.arrived(self.V.at[pl.ds(0, 7)], 6)
        total = self.V[0].astype(F32)
        for z in range(1, 8):
            total = total + self.V[z].astype(F32)
        self.E[...] = total.astype(BF16)
        for d in (2, 1, 3):
            self.start(self.E, self.O.at[at.y], 4, 7, at.at(dy=d))

    def stage6(self, write):
        at = self.place
        self.arrived(self.O.at[pl.ds(0, 3)], 7)
        self.O[at.y] = self.E[...]
        for r in range(2):
            for k in range(2):
                write(r, k, self.O[2 * r + k])

    def drain(self):
        self.left(self.R, 0)
        self.left(self.A.at[pl.ds(0, 3)], 1)
        self.left(self.A.at[0, pl.ds(0, 3)], 2)
        self.left(self.V.at[pl.ds(0, 7)], 3)
        self.left(self.O.at[pl.ds(0, 3)], 4)


SMALL_SEMS = (4, 4)


class Small(Copies):
    def __init__(self, place, tile, slots, send_sems, recv_sems):
        super().__init__(place, send_sems, recv_sems)
        self.tile, self.slots = tile, slots

    def step(self, n):
        at = self.place
        size, mine = ((4, at.x), (4, at.y), (8, at.z), (2, at.c))[n]
        other = (
            lambda d: at.at(dx=d),
            lambda d: at.at(dy=d),
            lambda d: at.at(dz=d),
            lambda d: at.sibling(),
        )[n]
        return size, mine, other

    def send(self, n):
        size, mine, other = self.step(n)
        for d in range(1, size):
            self.start(self.tile.at[n], self.slots.at[n, mine], n, n, other(d))

    def receive(self, n):
        size, mine, _ = self.step(n)
        self.arrived(self.slots.at[n, pl.ds(0, size - 1)], n)
        self.slots[n, mine] = self.tile[n]
        total = self.slots[n, 0].astype(F32)
        for k in range(1, size):
            total = total + self.slots[n, k].astype(F32)
        return total

    def stage0(self):
        self.send(0)

    def stage1(self):
        self.tile[1] = self.receive(0).astype(BF16)
        self.send(1)

    def stage2(self):
        self.tile[2] = self.receive(1).astype(BF16)
        self.send(2)

    def stage3(self):
        self.tile[3] = self.receive(2).astype(BF16)
        self.send(3)

    def stage4(self, write):
        write(self.receive(3))

    def drain(self):
        for n in range(4):
            self.left(self.slots.at[n, pl.ds(0, self.step(n)[0] - 1)], n)


class Timeline:
    def __init__(self):
        self.now, self.live = 0.0, []

    def add(self, stages, start=0.0, first=0.0):
        work = [max(start, self.now), first, len(self.live), list(stages)]
        self.live.append(work)
        self.run(self.now)
        return work

    def step(self, work):
        call, latency = work[3].pop(0)
        call()
        work[0] = max(self.now, work[0]) + latency

    def run(self, until):
        while True:
            ready = [w for w in self.live if w[3] and w[0] <= until]
            if not ready:
                return
            self.step(min(ready, key=lambda w: (w[0] - w[1], w[2])))

    def spend(self, time):
        self.now += time
        self.run(self.now)

    def finish(self, work):
        while work[3]:
            self.now = max(self.now, min(w[0] for w in self.live if w[3]))
            self.run(self.now)


SCRATCH = {
    "normed": ((384, 1024), F32),
    "inverse": ((384, 128), F32),
    "hidden": ((384, 1024), BF16),
    "hidden_t": ((1024, 384), BF16),
    "mcot": ((384, 1024), BF16),
    "live": ((384, 128), F32),
    "ga": ((4, 384, 256), BF16),
    "att": ((4, 384, 256), BF16),
    "qkv": ((2, 384, 768), BF16),
    "dqkv": ((4, 384, 768), BF16),
    "bias": ((384, 384), F32),
    "gains": ((2, 1024), F32),
    "probs": ((2, 4, 384, 384), F32),
    "low": ((2, 384, 384), BF16),
    "dscores": ((2, 384, 384), BF16),
    "gh": ((384, 1024), F32),
    "tokens": ((384, 1024), BF16),
    "cot": ((384, 1024), BF16),
    "own": ((128, 128), F32),
    "own_low": ((32, 128), BF16),
    "sums": ((16, 128), F32),
    "gain": ((1, 32), BF16),
    "shift": ((1, 32), BF16),
}


def own_small(S):
    S["own"][...] = jnp.zeros((128, 128), F32)
    S["own"][0:1, 0:32] = S["gain"][...].astype(F32)
    S["own"][1:2, 0:32] = S["shift"][...].astype(F32)
    S["own_low"][...] = S["own"][...].T[0:32].astype(BF16)


def prologue_tokens(S, count_ref, starts_ref):
    source = S["tokens"][...].astype(F32)
    center = jnp.mean(source, axis=1, keepdims=True)
    centered = source - center
    variance = jnp.mean(centered * centered, axis=1, keepdims=True)
    inverse = lax.rsqrt(variance + 1e-06)
    S["normed"][...] = centered * inverse
    S["inverse"][...] = jnp.broadcast_to(inverse, (ROWS, 128))
    count = count_ref[0]
    down = lax.broadcasted_iota(jnp.int32, (ROWS, 1), 0)
    across = lax.broadcasted_iota(jnp.int32, (1, ROWS), 1)
    seg_down = jnp.zeros((ROWS, 1), jnp.int32)
    seg_across = jnp.zeros((1, ROWS), jnp.int32)
    for j in range(8):
        start = starts_ref[0, j]
        seg_down = seg_down + jnp.where(down >= start, 1, 0)
        seg_across = seg_across + jnp.where(across >= start, 1, 0)
    seg_down = jnp.where(down < count, seg_down, -1)
    seg_across = jnp.where(across < count, seg_across, -2)
    S["bias"][...] = jnp.where(seg_down == seg_across, 0.0, -1e30).astype(F32)
    alive = lax.broadcasted_iota(jnp.int32, (ROWS, 128), 0) < count
    S["live"][...] = jnp.where(alive, 1.0, 0.0).astype(F32)
    alive = S["live"][:, 0:1] > 0.5
    S["mcot"][...] = jnp.where(alive, S["cot"][...].astype(F32), 0.0).astype(BF16)


def prologue_hidden(S):
    small = S["W0"][:, :, :, :, 768:896].reshape(1024, 128).astype(F32)
    S["gains"][...] = small.T[0:2, :]
    gain = S["gains"][0:1, :]
    shift = S["gains"][1:2, :]
    S["hidden"][...] = (S["normed"][...] * gain + shift).astype(BF16)
    S["hidden_t"][...] = S["hidden"][...].T


def grads_attended(S):
    for g in range(4):
        part = S["Wp"][g].reshape(256, 1024)
        S["ga"][g] = nt(S["mcot"][...], part).astype(BF16)


def own(a, h):
    first = lax.broadcasted_iota(jnp.int32, (ROWS, 128), 1) < 64
    zero = jnp.zeros_like(a)
    return jnp.where(first, a, zero) if h == 0 else jnp.where(first, zero, a)


def lanes(ref, pair, part):
    return ref[:, part * 256 + pair * 128 : part * 256 + pair * 128 + 128]


def forward(S, g, spend):
    qkv, slot = S["qkv"].at[g % 2], g % 2
    for n in range(3):
        weight = S[f"W{g}"][:, :, :, :, n * 256 : n * 256 + 256].reshape(1024, 256)
        part = nn(S["hidden"][...], weight).astype(BF16)
        qkv[:, n * 256 : n * 256 + 256] = part * jnp.asarray(0.125, BF16) if n == 0 else part
    spend(0.8)
    for pair in range(2):
        q2, k2, v2 = (lanes(qkv, pair, n) for n in range(3))
        for h in range(2):
            scores = nt(own(q2, h), k2) + S["bias"][...]
            row_max = jnp.max(scores, axis=1, keepdims=True)
            expon = jnp.exp(scores - row_max)
            probs = expon * (1.0 / jnp.sum(expon, axis=1, keepdims=True))
            S["probs"][slot, 2 * pair + h] = probs
            S["low"][h] = probs.astype(BF16)
        att = sum(nn(S["low"][h], own(v2, h)) for h in range(2))
        S["att"][g, :, pair * 128 : pair * 128 + 128] = att.astype(BF16)
        spend(0.85)


def backward(S, g, spend):
    qkv, slot = S["qkv"].at[g % 2], g % 2
    for pair in range(2):
        q2, k2, v2 = (lanes(qkv, pair, n) for n in range(3))
        o2 = S["ga"][g, :, pair * 128 : pair * 128 + 128]
        for h in range(2):
            probs = S["probs"][slot, 2 * pair + h]
            grad_probs = nt(own(o2, h), v2)
            delta = jnp.sum(probs * grad_probs, axis=1, keepdims=True)
            S["dscores"][h] = (probs * (grad_probs - delta)).astype(BF16)
            S["low"][h] = probs.astype(BF16)
        spend(0.55)
        dv = sum(tn(S["low"][h], own(o2, h)) for h in range(2))
        dq = sum(nn(S["dscores"][h], own(k2, h)) for h in range(2)) * 0.125
        dk = sum(tn(S["dscores"][h], own(q2, h)) for h in range(2))
        for n, part in enumerate((dq, dk, dv)):
            start = n * 256 + pair * 128
            S["dqkv"][g, :, start : start + 128] = part.astype(BF16)
        spend(0.55)


def weight_grads(S, g, spend):
    for m in range(4):
        if m:
            spend(0.25)
        part = nn(S["hidden_t"][m * 256 : m * 256 + 256], S["dqkv"][g]).astype(BF16)
        part = part.reshape(4, 2, 2, 16, 768)
        for r in range(2):
            for k in range(2):
                S["G"][g, m, :, :, 2 * r + k] = part[:, :, r, :, k * 384 : k * 384 + 384]


def hidden_grads(S, spend):
    for n in range(4):
        S["gh"][:, n * 256 : n * 256 + 256] = sum(
            nt(S["dqkv"][g], S[f"W{g}"][n, :, :, :, 0:768].reshape(256, 768)) for g in range(4)
        )
        spend(1.15)


def proj_grads(S):
    for g in range(4):
        part = tn(S["att"][g], S["mcot"][...]).astype(BF16).reshape(4, 2, 2, 16, 1024)
        for r in range(2):
            for k in range(2):
                S["Gp"][g, :, :, 2 * r + k] = part[:, :, r, :, k * 512 : k * 512 + 512]


def small_grads(S):
    gh = S["gh"][...]
    gain_term = jnp.sum(gh * S["normed"][...], axis=0, keepdims=True)
    shift_term = jnp.sum(gh, axis=0, keepdims=True)
    for r in range(8):
        S["sums"][r : r + 1, :] = gain_term[:, r * 128 : r * 128 + 128]
        S["sums"][8 + r : 9 + r, :] = shift_term[:, r * 128 : r * 128 + 128]
    S["tile"][0] = S["sums"][...].astype(BF16)


def token_grads(S):
    normed = S["normed"][...]
    grad_normed = S["gh"][...] * S["gains"][0:1, :]
    inner = grad_normed - jnp.mean(grad_normed, axis=1, keepdims=True)
    inner = inner - normed * jnp.mean(grad_normed * normed, axis=1, keepdims=True)
    S["tokens"][...] = (S["cot"][...].astype(F32) + S["inverse"][:, 0:1] * inner).astype(BF16)


COMM = {}
for _name, _shape in reduce_shapes(384).items():
    COMM["g_" + _name] = ((4,) + _shape, BF16)
for _name, _shape in reduce_shapes(512).items():
    COMM["p_" + _name] = (_shape, BF16)
for _g, _width in enumerate((896, 768, 768, 768)):
    COMM[f"W{_g}"] = ((4, 4, 2, 32, _width), BF16)
COMM["Wp"] = ((4, 4, 2, 32, 1024), BF16)
COMM["G"] = ((4, 4, 4, 2, 4, 16, 384), BF16)
COMM["Gp"] = ((4, 4, 2, 4, 16, 512), BF16)
COMM["tile"] = ((4, 16, 128), BF16)
COMM["slots"] = ((4, 8, 16, 128), BF16)


def kernel(
    count_ref,
    starts_ref,
    tok_ref,
    cot_ref,
    qkv_ref,
    proj_ref,
    gain_ref,
    shift_ref,
    out_ref,
    qkv_out,
    proj_out,
    gain_out,
    shift_out,
    *scratch,
):
    S = dict(zip(tuple(SCRATCH) + tuple(COMM), scratch))
    gs, gr, rs, rr, ss, sr, ls, count, starts = scratch[len(S) :]
    place = Place()
    x, z, c = place.x, place.zlo, place.c
    time = Timeline()

    def prepare():
        few = (count_ref, count), (starts_ref, starts), (gain_ref, S["gain"]), (shift_ref, S["shift"])
        few = [pltpu.make_async_copy(a, b, ls.at[8 + n]) for n, (a, b) in enumerate(few)]
        for copy in few:
            copy.start()
        into = [(tok_ref, S["tokens"]), (cot_ref, S["cot"]), (proj_ref, S["Wp"].at[x, z, c])]
        into = [pltpu.make_async_copy(a, b, ls.at[n]) for n, (a, b) in enumerate(into)]
        for copy in into:
            copy.start()
        for g in range(4):
            for part in range(3):
                pltpu.make_async_copy(
                    qkv_ref.at[:, pl.ds(part * 1024 + g * 256, 256)],
                    S[f"W{g}"].at[x, z, c, :, pl.ds(part * 256, 256)],
                    ls.at[3 + g],
                ).start()
        for copy in few:
            copy.wait()
        own_small(S)
        last = S["W0"].at[x, z, c, :, pl.ds(768, 128)]
        last = pltpu.make_async_copy(S["own_low"], last, ls.at[7])
        last.start()
        into[0].wait()
        into[1].wait()
        prologue_tokens(S, count, starts)
        into[2].wait()
        last.wait()
        for g in range(4):
            own = S[f"W{g}"].at[x, z, c, :, pl.ds(0, 768)]
            pltpu.make_async_copy(own, own, ls.at[3 + g]).wait()

    enter(place.all(), prepare)

    buffers = [S[f"W{g}"] for g in range(4)] + [S["Wp"]]
    gathers = [Gather(place, b, k in DIRECT, gs.at[k], gr.at[k]) for k, b in enumerate(buffers)]

    def gather(k, start):
        piece = gathers[k]
        calls = (piece.stage0, piece.stage1, piece.stage2, piece.stage3, piece.stage4, piece.stage5)
        return time.add(zip(calls, DIRECT_TIMES if piece.direct else GATHER_TIMES), start)

    def write_group(g):
        def write(r, k, value):
            rows = slice(r * 16, r * 16 + 16)
            if k == 0:
                qkv_out[rows, g * 256 : g * 256 + 256] = value[:, 0:256]
                qkv_out[rows, 1024 + g * 256 : 1152 + g * 256] = value[:, 256:384]
            else:
                qkv_out[rows, 1152 + g * 256 : 1280 + g * 256] = value[:, 0:128]
                qkv_out[rows, 2048 + g * 256 : 2304 + g * 256] = value[:, 128:384]

        return write

    def write_proj(r, k, value):
        proj_out[r * 16 : r * 16 + 16, k * 512 : k * 512 + 512] = value

    def write_small(total):
        S["sums"][...] = total
        place_in_row = place.zlo * 2 + place.c
        for first, out in ((0, gain_out), (8, shift_out)):
            row = S["sums"][pl.ds(first + place.x * 2 + place.zlo // 2, 1), :]
            value = jnp.zeros((1, 32), F32)
            for k in range(4):
                value = jnp.where(place_in_row % 4 == k, row[:, k * 32 : k * 32 + 32], value)
            out[...] = value

    reduces = []

    def reduce(term, names, sem, write):
        piece = Reduce(place, term, names, rs.at[sem], rr.at[sem])
        reduces.append(piece)
        calls = (piece.stage0, piece.stage1, piece.stage2, piece.stage3, piece.stage4)
        calls += (piece.stage5, functools.partial(piece.stage6, write))
        final = sem == 3
        return time.add(zip(calls, REDUCE_TIMES[sem]), 0.0, 1.5 if final else 0.0)

    works = dict((k, gather(k, start)) for k, start in GATHER_STARTS)
    time.finish(works[0])
    prologue_hidden(S)
    time.spend(0.5)
    forward(S, 0, time.spend)
    time.finish(works[4])
    grads_attended(S)
    time.spend(1.0)
    for g in range(4):
        if 0 < g < 3:
            time.finish(works[g + 1])
            forward(S, g + 1, time.spend)
        if g == 2:
            proj_grads(S)
            reduce(S["Gp"], [S["p_" + n] for n in REDUCE_NAMES], 4, write_proj)
            time.spend(1.3)
        backward(S, g, time.spend)
        weight_grads(S, g, time.spend)
        names = [S["g_" + n].at[g] for n in REDUCE_NAMES]
        reduce(S["G"].at[g], names, g, write_group(g))
        time.spend(0.25)
        if g == 0:
            time.finish(works[1])
            forward(S, 1, time.spend)
    hidden_grads(S, time.spend)
    small_grads(S)
    small = Small(place, S["tile"], S["slots"], ss, sr)
    calls = (small.stage0, small.stage1, small.stage2, small.stage3)
    calls += (functools.partial(small.stage4, write_small),)
    time.add(zip(calls, SMALL_TIMES), 0.0, 1.0)
    time.spend(0.3)
    token_grads(S)
    out = pltpu.make_async_copy(S["tokens"], out_ref, ls.at[0])
    out.start()
    time.spend(0.8)
    for work in list(time.live):
        time.finish(work)
    out.wait()
    for piece in gathers + reduces + [small]:
        piece.drain()


GATHER_STARTS = ((0, 0.0), (4, 3.4), (1, 7.0), (2, 10.0), (3, 13.5))
DIRECT = (0, 4)
DIRECT_TIMES = (3.4, 0.8, 6.0, 0.9, 2.0, 0.0)
GATHER_TIMES = (3.6, 0.8, 4.5, 4.0, 2.0, 0.0)
EARLY = (2.5, 4.8, 5.0, 5.0, 5.5, 30.0, 0.0)
LATE = (2.0, 4.5, 5.5, 5.5, 5.0, 30.0, 0.0)
FINAL = (1.1, 4.3, 4.8, 4.2, 4.6, 30.0, 0.0)
REDUCE_TIMES = (EARLY, EARLY, LATE, FINAL, (4.3,) + LATE[1:])
SMALL_TIMES = (4.4, 4.6, 5.6, 25.0, 0.0)


LAST_SHAPES = (
    (ROWS, D, BF16, BF16),
    (32, 3072, BF16, F32),
    (32, 1024, BF16, F32),
    (1, 32, F32, F32),
    (1, 32, F32, F32),
)


def last_kernel(scale, *refs):
    ins, outs, scratch, sems = refs[:5], refs[5:10], refs[10:-1], refs[-1]
    before = scratch[:5]
    after = (scratch[0],) + scratch[5:]
    into = [pltpu.make_async_copy(a, b, sems.at[n]) for n, (a, b) in enumerate(zip(ins, before))]
    out = [pltpu.make_async_copy(a, b, sems.at[5 + n]) for n, (a, b) in enumerate(zip(after, outs))]
    for copy in into:
        copy.start()
    for n in (1, 2, 3, 4, 0):
        into[n].wait()
        if n:
            after[n][...] = before[n][...].astype(F32) * scale
        out[n].start()
    for copy in out:
        copy.wait()


def last(scale, *arrays):
    anyspace = pl.BlockSpec(memory_space=pl.ANY)
    return pl.pallas_call(
        functools.partial(last_kernel, scale),
        out_shape=[jax.ShapeDtypeStruct((r, c), t) for r, c, _, t in LAST_SHAPES],
        in_specs=[anyspace] * 5,
        out_specs=[anyspace] * 5,
        scratch_shapes=[pltpu.VMEM((r, c), t) for r, c, t, _ in LAST_SHAPES]
        + [pltpu.VMEM((r, c), t) for r, c, _, t in LAST_SHAPES[1:]]
        + [pltpu.SemaphoreType.DMA((10,))],
        name="last",
    )(*arrays)


def fused(counts, starts, tokens, cotangent, qkv_weight, proj_weight, gain, shift):
    anyspace = pl.BlockSpec(memory_space=pl.ANY)
    vmem = pl.BlockSpec(memory_space=pltpu.VMEM)
    buffers = tuple(SCRATCH.values()) + tuple(COMM.values())
    return pl.pallas_call(
        kernel,
        out_shape=[
            jax.ShapeDtypeStruct((ROWS, D), BF16),
            jax.ShapeDtypeStruct((32, 3072), BF16),
            jax.ShapeDtypeStruct((32, 1024), BF16),
            jax.ShapeDtypeStruct((1, 32), F32),
            jax.ShapeDtypeStruct((1, 32), F32),
        ],
        in_specs=[anyspace] * 8,
        out_specs=[anyspace] + [vmem] * 4,
        scratch_shapes=[pltpu.VMEM(*b) for b in buffers]
        + [
            pltpu.SemaphoreType.DMA((5, GATHER_SEMS[0])),
            pltpu.SemaphoreType.DMA((5, GATHER_SEMS[1])),
            pltpu.SemaphoreType.DMA((5, REDUCE_SEMS[0])),
            pltpu.SemaphoreType.DMA((5, REDUCE_SEMS[1])),
            pltpu.SemaphoreType.DMA((SMALL_SEMS[0],)),
            pltpu.SemaphoreType.DMA((SMALL_SEMS[1],)),
            pltpu.SemaphoreType.DMA((12,)),
            pltpu.SMEM((1,), jnp.int32),
            pltpu.SMEM((1, 8), jnp.int32),
        ],
        compiler_params=pltpu.CompilerParams(
            collective_id=0, has_side_effects=True, vmem_limit_bytes=67043328
        ),
        name="fused",
    )(counts, starts, tokens, cotangent, qkv_weight, proj_weight, gain, shift)


def per_device(
    tokens, cotangent, patch_count, image_starts, qkv_weight, proj_weight, norm_gain, norm_shift
):
    everyone = lax.axis_size("dp") * lax.axis_size("fsdp")
    scale = 1.0 / math.sqrt(tokens.shape[0] * everyone)
    sums = fused(
        patch_count,
        image_starts,
        tokens,
        cotangent,
        qkv_weight,
        proj_weight,
        norm_gain.reshape(1, -1),
        norm_shift.reshape(1, -1),
    )
    grad_block, qkv_grad, proj_grad, gain_grad, shift_grad = last(scale, *sums)
    return (grad_block, qkv_grad, proj_grad, gain_grad.reshape(-1), shift_grad.reshape(-1))


def solution(mesh):
    placed = (
        P(("dp", "fsdp"), None),
        P(("dp", "fsdp"), None),
        P(("dp", "fsdp")),
        P(("dp", "fsdp"), None),
        P("fsdp", None),
        P("fsdp", None),
        P("fsdp"),
        P("fsdp"),
    )
    return jax.shard_map(
        per_device,
        mesh=mesh,
        in_specs=placed,
        out_specs=(P(("dp", "fsdp"), None), P("fsdp", None), P("fsdp", None), P("fsdp"), P("fsdp")),
        check_vma=False,
    )
```
